32 devices in a mesh: dp: 8 (over z, core), tp: 4 (over y, x).
Axes of the slice: x: 2, y: 2, z: 4, core: 2. Of those that a mesh axis runs over, the one named last changes fastest.
Arguments:
- master: float32 [4096, 10240], P(('dp', 'tp')), may hold values from -0.09375 to 0.09375
- grad: float32 [4096, 10240], P(('dp', 'tp')), may hold values from -0.006 to 0.006
- exp_avg: float32 [4096, 10240], P(('dp', 'tp')), may hold values from -0.006 to 0.006
- exp_avg_sq: float32 [4096, 10240], P(('dp', 'tp')), may hold values from 1e-08 to 1e-05
Outputs:
- new_master: float32 [4096, 10240], P(('dp', 'tp'))
- new_avg: float32 [4096, 10240], P(('dp', 'tp'))
- new_avg_sq: float32 [4096, 10240], P(('dp', 'tp'))
- engine_qkv: bfloat16 [4096, 10240], P(None, 'tp')
The draws below stay inside these ranges and needn't reach their ends.
All inputs are finite; a program needn't handle non-finite values.
Results may differ from the reference program's by a relative error of at most 0.001.
Values may be sent and summed in bfloat16 or wider, within the bound.
A program may use at most 128 MiB of HBM per device.

```python
import math
import jax
import jax.numpy as jnp

QH = 64
KVH = 8
HS = 128
D_WIN = 4096
QKVW = 10240
N_TP = 4


def level_of(own_key, dims, pieces, smallest, top_value):
    def one(position, shards_of):
        heights = jax.random.uniform(jax.random.fold_in(jax.random.fold_in(own_key, 6), position), (shards_of,), jnp.float32, smallest / len(pieces), top_value / len(pieces))
        return jnp.repeat(jnp.exp(heights), dims[position] // shards_of).reshape((-1,) + (1,) * (len(dims) - position - 1))

    gain = one(*pieces[0])
    for cut in pieces[1:]:
        gain = gain * one(*cut)
    return gain


def scatter_about(rng, extent, width, most, shards=(), dtype=jnp.bfloat16):
    array = jax.random.normal(rng, extent, jnp.float32) * width
    if len(shards) > 0:
        array = level_of(rng, extent, shards, -0.22, 0.18) * array
    return jnp.clip(array, min=-most, max=most).astype(dtype)


def setup_inputs(seed: int = 0) -> dict:
    arg_keys = jax.random.split(jax.random.key(seed), 5)
    return {
        "master": scatter_about(arg_keys[0], (D_WIN, QKVW), D_WIN ** -0.5, 0.09375, ((0, 32),), jnp.float32),
        "grad": scatter_about(arg_keys[1], (D_WIN, QKVW), 0.001, 0.006, ((0, 32),), jnp.float32),
        "exp_avg": scatter_about(arg_keys[2], (D_WIN, QKVW), 0.001, 0.006, ((0, 32),), jnp.float32),
        "exp_avg_sq": jnp.clip(jnp.exp(math.log(9.999999747378752e-06) - 6.9077553 * jax.random.uniform(arg_keys[3], (D_WIN, QKVW), jnp.float32) ** level_of(arg_keys[3], (D_WIN, QKVW), ((0, 32),), -0.2, 0.2)), 9.99999993922529e-09, 9.999999747378752e-06),
    }


def joined_slices(weights, tp_count):
    rows = weights.shape[0]
    query = weights[:, :QH * HS].reshape(rows, tp_count, QH // tp_count * HS)
    keys = weights[:, QH * HS:(QH + KVH) * HS].reshape(rows, tp_count, KVH // tp_count * HS)
    values = weights[:, (QH + KVH) * HS:].reshape(rows, tp_count, KVH // tp_count * HS)
    return jnp.concatenate([query, keys, values], axis=2).reshape(rows, -1)

def reference(master, grad, exp_avg, exp_avg_sq):
    corr_one = 1.0 - 0.9 ** 10
    corr_two = 1.0 - 0.999 ** 10
    new_avg = 0.9 * exp_avg + 0.1 * grad
    new_avg_sq = 0.999 * exp_avg_sq + 0.001 * grad * grad
    update = new_avg / corr_one / (jnp.sqrt(new_avg_sq / corr_two) + 1e-08)
    new_master = master - 0.001 * (update + 0.1 * master)
    engine_qkv = joined_slices(new_master, N_TP).astype(jnp.bfloat16)
    return (new_master, new_avg, new_avg_sq, engine_qkv)
```

```python
import functools

import jax
import jax.numpy as jnp
from jax import lax
from jax.experimental import pallas as pl
from jax.experimental.pallas import tpu as pltpu
from jax.sharding import PartitionSpec as P

QH = 64
KVH = 8
HS = 128
CORES = 2
STEP = 16
MESH = pl.DeviceIdType.MESH


def step_math(master, grad, exp_avg, exp_avg_sq):
    corr_one = 1.0 - 0.9**10
    corr_two = 1.0 - 0.999**10
    new_avg = 0.9 * exp_avg + 0.1 * grad
    new_avg_sq = 0.999 * exp_avg_sq + 0.001 * grad * grad
    update = new_avg / corr_one / (jnp.sqrt(new_avg_sq / corr_two) + 1e-08)
    new_master = master - 0.001 * (update + 0.1 * master)
    return new_master, new_avg, new_avg_sq


def pieces_of(tp_count, t):
    q, kv = QH // tp_count * HS, KVH // tp_count * HS
    return [(t * q, q, 0), (QH * HS + t * kv, kv, q), ((QH + KVH) * HS + t * kv, kv, q + kv)]


def mix(t, j, count):
    out, bit = 0, 1
    while bit < count:
        out = out + ((t // bit) % 2 + (j // bit) % 2) % 2 * bit
        bit *= 2
    return out


def parts_of(rows):
    return 2 if rows % 64 == 0 else 1


def jobs_of(tp_count, rows):
    part_rows = rows // parts_of(rows)
    jobs, start = [], 0
    first = [STEP, STEP]
    while sum(first) < part_rows:
        first.append(min(sum(first), part_rows - sum(first)))
    for size in first + [part_rows] * (rows // part_rows - 1):
        jobs.append((0, start, size))
        start += size
    for j in range(1, tp_count):
        for h in range(rows // part_rows):
            jobs.append((j, h * part_rows, part_rows))
    return jobs


def spread_kernel(dp_count, tp_count, parts, *refs):
    sources, out_ref, held, mine, load_sem = refs[:4], refs[4], refs[5], refs[6], refs[7]
    own_sem, flat_send, up_send, down_send, side_send, in_recv, side_recv = refs[8:]
    planes = dp_count // CORES
    dp, t = lax.axis_index("dp"), lax.axis_index("tp")
    z, core = dp // CORES, dp % CORES
    rows = mine.shape[1]
    part_rows = rows // parts
    has_up, has_down = z < planes - 1, z > 0
    units = tp_count * parts

    up = {"dp": dp + CORES}
    down = {"dp": dp - CORES}
    side = {"dp": z * CORES + 1 - core}

    barrier = pltpu.get_barrier_semaphore()
    for j in range(1, tp_count):
        pl.semaphore_signal(barrier, inc=1, device_id={"tp": mix(t, j, tp_count)}, device_id_type=MESH)
    pl.semaphore_signal(barrier, inc=1, device_id=side, device_id_type=MESH)

    @pl.when(has_up)
    def _():
        pl.semaphore_signal(barrier, inc=1, device_id=up, device_id_type=MESH)

    @pl.when(has_down)
    def _():
        pl.semaphore_signal(barrier, inc=1, device_id=down, device_id_type=MESH)

    jobs = jobs_of(tp_count, rows)

    def loads(i):
        j, first, size = jobs[i]
        part = pl.ds(first, size)
        return [
            pltpu.make_async_copy(
                sources[n].at[part, pl.ds(pl.multiple_of(start, HS), width)],
                held.at[j, n, part, pl.ds(into, width)],
                load_sem.at[(i * 4 + n) * 3 + k],
            )
            for n in range(4)
            for k, (start, width, into) in enumerate(pieces_of(tp_count, mix(t, j, tp_count)))
        ]

    def compute(i):
        j, first, size = jobs[i]

        def rows_at(start):
            part = pl.ds(start, STEP)
            new_master = step_math(*[held[j, n, part, :] for n in range(4)])[0]
            mine[j, part, :] = new_master.astype(jnp.bfloat16)

        if size == STEP:
            rows_at(first)
        else:

            @pl.loop(0, size // STEP)
            def _(k):
                rows_at(pl.multiple_of(first + k * STEP, STEP))

    def place(plane, which_core, unit):
        source = mix(t, unit // parts, tp_count)
        block = (plane * CORES + which_core) * tp_count + source
        start = block * rows + unit % parts * part_rows
        return out_ref.at[pl.ds(pl.multiple_of(start, part_rows), part_rows), :]

    def copy(src, dst, send, recv, target):
        return pltpu.make_async_remote_copy(
            src_ref=src, dst_ref=dst, send_sem=send, recv_sem=recv, device_id=target, device_id_type=MESH
        )

    def going_up(src, dst, plane, unit):
        return copy(src, dst, up_send.at[plane, unit], in_recv.at[plane, unit], up)

    def going_down(src, dst, plane, unit):
        return copy(src, dst, down_send.at[plane, unit], in_recv.at[plane, unit], down)

    def going_side(src, dst, plane, unit):
        return copy(src, dst, side_send.at[plane, unit], side_recv.at[plane, unit], side)

    def arrived(plane, unit):
        here = place(plane, core, unit)
        copy(here, here, side_send.at[plane, unit], in_recv.at[plane, unit], side).wait_recv()

    def home(first, size):
        start = ((z * CORES + core) * tp_count + t) * rows + first
        return out_ref.at[pl.ds(pl.multiple_of(start, STEP), size), :]

    def flat_copy(j, h):
        part = pl.ds(h * part_rows, part_rows)
        unit = j * parts + h
        target = {"tp": mix(t, j, tp_count)}
        return copy(mine.at[j, part, :], home(h * part_rows, part_rows), flat_send.at[unit], in_recv.at[z, unit], target)

    def keep(h):
        return pltpu.make_async_copy(mine.at[0, pl.ds(h * part_rows, part_rows), :], place(z, core, h), own_sem.at[h])

    def send(i):
        j, first, size = jobs[i]
        h = first // part_rows
        if j > 0:
            flat_copy(j, h).start()
            return
        src, dst = mine.at[0, pl.ds(first, size), :], home(first, size)

        @pl.when(has_up)
        def _():
            going_up(src, dst, z, h).start()

        @pl.when(has_down)
        def _():
            going_down(src, dst, z, h).start()

        going_side(src, dst, z, h).start()
        if (first + size) % part_rows == 0:
            keep(h).start()

    ahead = 2
    for i in range(ahead):
        for cp in loads(i):
            cp.start()
    for i in range(len(jobs)):
        for cp in loads(i):
            cp.wait()
        if i + ahead < len(jobs):
            for cp in loads(i + ahead):
                cp.start()
        compute(i)
        if i == 0:
            pl.semaphore_wait(barrier, tp_count + has_up.astype(jnp.int32) + has_down.astype(jnp.int32))
        else:
            send(i - 1)
    send(len(jobs) - 1)

    @pl.loop(parts, units)
    def _(unit):
        arrived(z, unit)
        here = place(z, core, unit)

        @pl.when(has_up)
        def _():
            going_up(here, here, z, unit).start()

        @pl.when(has_down)
        def _():
            going_down(here, here, z, unit).start()

        going_side(here, here, z, unit).start()

    @pl.loop(0, (planes - 1) * units)
    def _(m):
        distance, unit = m // units + 1, m % units
        below, above = z - distance, z + distance

        @pl.when(below >= 0)
        def _():
            arrived(below, unit)
            here = place(below, core, unit)

            @pl.when(has_up)
            def _():
                going_up(here, here, below, unit).start()

            going_side(here, here, below, unit).start()

        @pl.when(above < planes)
        def _():
            arrived(above, unit)
            here = place(above, core, unit)

            @pl.when(has_down)
            def _():
                going_down(here, here, above, unit).start()

            going_side(here, here, above, unit).start()

    for h in range(parts):
        keep(h).wait()
    for j in range(1, tp_count):
        for h in range(parts):
            flat_copy(j, h).wait_send()

    @pl.loop(0, planes * units)
    def _(m):
        plane, unit = m // units, m % units
        here = place(plane, core, unit)
        there = place(plane, 1 - core, unit)

        @pl.when((plane <= z) & has_up)
        def _():
            going_up(here, here, plane, unit).wait_send()

        @pl.when((plane >= z) & has_down)
        def _():
            going_down(here, here, plane, unit).wait_send()

        going_side(here, here, plane, unit).wait_send()
        copy(there, there, side_send.at[plane, unit], side_recv.at[plane, unit], side).wait_recv()


def spread(dp_count, tp_count, *arrays):
    rows, cols = arrays[0].shape
    width = cols // tp_count
    parts = parts_of(rows)
    planes, units = dp_count // CORES, tp_count * parts
    grid = pltpu.SemaphoreType.DMA((planes, units))
    jobs = len(jobs_of(tp_count, rows))
    return pl.pallas_call(
        functools.partial(spread_kernel, dp_count, tp_count, parts),
        in_specs=[pl.BlockSpec(memory_space=pltpu.HBM)] * 4,
        out_specs=pl.BlockSpec(memory_space=pl.ANY),
        out_shape=pltpu.VMEM((dp_count * tp_count * rows, width), jnp.bfloat16),
        scratch_shapes=[
            pltpu.VMEM((tp_count, 4, rows, width), jnp.float32),
            pltpu.VMEM((tp_count, rows, width), jnp.bfloat16),
            pltpu.SemaphoreType.DMA((jobs * 12,)),
            pltpu.SemaphoreType.DMA((parts,)),
            pltpu.SemaphoreType.DMA((units,)),
        ]
        + [grid] * 5,
        compiler_params=pltpu.CompilerParams(collective_id=0, has_side_effects=True, vmem_limit_bytes=28 * 2**20),
        cost_estimate=pl.CostEstimate(flops=20 * rows * cols, bytes_accessed=16 * rows * cols, transcendentals=rows * cols),
    )(*[pltpu.with_memory_space_constraint(x, pltpu.HBM) for x in arrays])


def step_kernel(m_ref, g_ref, a_ref, s_ref, all_ref, nm_ref, na_ref, ns_ref, engine_ref, sems):
    count = sems.shape[0]
    rows = engine_ref.shape[0] // count

    def whole(n):
        part = pl.ds(n * rows, rows)
        return pltpu.make_async_copy(all_ref.at[part, :], engine_ref.at[part, :], sems.at[n])

    @pl.when(pl.program_id(0) == 0)
    def _():
        for n in range(count):
            whole(n).start()

    new_master, new_avg, new_avg_sq = step_math(m_ref[...], g_ref[...], a_ref[...], s_ref[...])
    nm_ref[...] = new_master
    na_ref[...] = new_avg
    ns_ref[...] = new_avg_sq

    @pl.when(pl.program_id(0) == pl.num_programs(0) - 1)
    def _():
        for n in range(count):
            whole(n).wait()


def local_step(arrays, gathered):
    rows, cols = arrays[0].shape
    tile = 16
    flat = pl.BlockSpec((tile, cols), lambda i: (i, 0))
    f32 = jax.ShapeDtypeStruct((rows, cols), jnp.float32)
    return pl.pallas_call(
        step_kernel,
        grid=(rows // tile,),
        in_specs=[flat] * 4 + [pl.BlockSpec(memory_space=pl.ANY)],
        out_specs=[flat] * 3 + [pl.BlockSpec(memory_space=pltpu.HBM)],
        out_shape=[f32] * 3 + [jax.ShapeDtypeStruct(gathered.shape, gathered.dtype)],
        scratch_shapes=[pltpu.SemaphoreType.DMA((4,))],
        compiler_params=pltpu.CompilerParams(vmem_limit_bytes=24 * 2**20),
        cost_estimate=pl.CostEstimate(
            flops=20 * rows * cols,
            bytes_accessed=28 * rows * cols + 2 * gathered.size,
            transcendentals=rows * cols,
        ),
    )(*[pltpu.with_memory_space_constraint(x, pltpu.HBM) for x in arrays], pltpu.with_memory_space_constraint(gathered, pltpu.VMEM))


def body(dp_count, tp_count, *arrays):
    gathered = spread(dp_count, tp_count, *arrays)
    return tuple(local_step(arrays, gathered))


def solution(mesh):
    flat = P(("dp", "tp"), None)
    return jax.shard_map(
        functools.partial(body, mesh.shape["dp"], mesh.shape["tp"]),
        mesh=mesh,
        in_specs=(flat,) * 4,
        out_specs=(flat, flat, flat, P(None, "tp")),
        check_vma=False,
    )
```

```python
import functools

import jax
import jax.numpy as jnp
from jax import lax
from jax.experimental import pallas as pl
from jax.experimental.pallas import tpu as pltpu
from jax.sharding import PartitionSpec as P

QH = 64
KVH = 8
HS = 128
CORES = 2
STEP = 16
MESH = pl.DeviceIdType.MESH


def step_math(master, grad, exp_avg, exp_avg_sq):
    corr_one = 1.0 - 0.9**10
    corr_two = 1.0 - 0.999**10
    new_avg = 0.9 * exp_avg + 0.1 * grad
    new_avg_sq = 0.999 * exp_avg_sq + 0.001 * grad * grad
    update = new_avg / corr_one / (jnp.sqrt(new_avg_sq / corr_two) + 1e-08)
    new_master = master - 0.001 * (update + 0.1 * master)
    return new_master, new_avg, new_avg_sq


def pieces_of(tp_count, t):
    q, kv = QH // tp_count * HS, KVH // tp_count * HS
    return [(t * q, q, 0), (QH * HS + t * kv, kv, q), ((QH + KVH) * HS + t * kv, kv, q + kv)]


def mix(t, j, count):
    out, bit = 0, 1
    while bit < count:
        out = out + ((t // bit) % 2 + (j // bit) % 2) % 2 * bit
        bit *= 2
    return out


def parts_of(rows):
    return 2 if rows % 64 == 0 else 1


def jobs_of(tp_count, rows):
    part_rows = rows // parts_of(rows)
    jobs, start = [], 0
    first = [STEP, STEP]
    while sum(first) < part_rows:
        first.append(min(sum(first), part_rows - sum(first)))
    for size in first + [part_rows] * (rows // part_rows - 1):
        jobs.append((0, start, size))
        start += size
    for j in range(1, tp_count):
        for h in range(rows // part_rows):
            jobs.append((j, h * part_rows, part_rows))
    return jobs


def spread_kernel(dp_count, tp_count, parts, late, *refs):
    sources, (out_ref, late_ref), (held, mine, load_sem) = refs[:4], refs[4:6], refs[6:9]
    own_sem, late_sem, flat_send, up_send, down_send, side_send, in_recv, side_recv = refs[9:]
    planes = dp_count // CORES
    dp, t = lax.axis_index("dp"), lax.axis_index("tp")
    z, core = dp // CORES, dp % CORES
    rows = mine.shape[1]
    part_rows = rows // parts
    has_up, has_down = z < planes - 1, z > 0
    units = tp_count * parts

    up = {"dp": dp + CORES}
    down = {"dp": dp - CORES}
    side = {"dp": z * CORES + 1 - core}

    barrier = pltpu.get_barrier_semaphore()
    for j in range(1, tp_count):
        pl.semaphore_signal(barrier, inc=1, device_id={"tp": mix(t, j, tp_count)}, device_id_type=MESH)
    pl.semaphore_signal(barrier, inc=1, device_id=side, device_id_type=MESH)

    @pl.when(has_up)
    def _():
        pl.semaphore_signal(barrier, inc=1, device_id=up, device_id_type=MESH)

    @pl.when(has_down)
    def _():
        pl.semaphore_signal(barrier, inc=1, device_id=down, device_id_type=MESH)

    jobs = jobs_of(tp_count, rows)

    def loads(i):
        j, first, size = jobs[i]
        part = pl.ds(first, size)
        return [
            pltpu.make_async_copy(
                sources[n].at[part, pl.ds(pl.multiple_of(start, HS), width)],
                held.at[j, n, part, pl.ds(into, width)],
                load_sem.at[(i * 4 + n) * 3 + k],
            )
            for n in range(4)
            for k, (start, width, into) in enumerate(pieces_of(tp_count, mix(t, j, tp_count)))
        ]

    def compute(i):
        j, first, size = jobs[i]

        def rows_at(start):
            part = pl.ds(start, STEP)
            new_master = step_math(*[held[j, n, part, :] for n in range(4)])[0]
            mine[j, part, :] = new_master.astype(jnp.bfloat16)

        if size == STEP:
            rows_at(first)
        else:

            @pl.loop(0, size // STEP)
            def _(k):
                rows_at(pl.multiple_of(first + k * STEP, STEP))

    def place(plane, which_core, unit):
        source = mix(t, unit // parts, tp_count)
        block = (plane * CORES + which_core) * tp_count + source
        start = block * rows + unit % parts * part_rows
        return out_ref.at[pl.ds(pl.multiple_of(start, part_rows), part_rows), :]

    def copy(src, dst, send, recv, target):
        return pltpu.make_async_remote_copy(
            src_ref=src, dst_ref=dst, send_sem=send, recv_sem=recv, device_id=target, device_id_type=MESH
        )

    def going_up(src, dst, plane, unit):
        return copy(src, dst, up_send.at[plane, unit], in_recv.at[plane, unit], up)

    def going_down(src, dst, plane, unit):
        return copy(src, dst, down_send.at[plane, unit], in_recv.at[plane, unit], down)

    def going_side(src, dst, plane, unit):
        return copy(src, dst, side_send.at[plane, unit], side_recv.at[plane, unit], side)

    def arrived(plane, unit):
        here = place(plane, core, unit)
        copy(here, here, side_send.at[plane, unit], in_recv.at[plane, unit], side).wait_recv()

    def home(first, size):
        start = ((z * CORES + core) * tp_count + t) * rows + first
        return out_ref.at[pl.ds(pl.multiple_of(start, STEP), size), :]

    def flat_copy(j, h):
        part = pl.ds(h * part_rows, part_rows)
        unit = j * parts + h
        target = {"tp": mix(t, j, tp_count)}
        return copy(mine.at[j, part, :], home(h * part_rows, part_rows), flat_send.at[unit], in_recv.at[z, unit], target)

    def keep(h):
        return pltpu.make_async_copy(mine.at[0, pl.ds(h * part_rows, part_rows), :], place(z, core, h), own_sem.at[h])

    def send(i):
        j, first, size = jobs[i]
        h = first // part_rows
        if j > 0:
            flat_copy(j, h).start()
            return
        src, dst = mine.at[0, pl.ds(first, size), :], home(first, size)

        @pl.when(has_up)
        def _():
            going_up(src, dst, z, h).start()

        @pl.when(has_down)
        def _():
            going_down(src, dst, z, h).start()

        going_side(src, dst, z, h).start()
        if (first + size) % part_rows == 0:
            keep(h).start()

    ahead = 2
    for i in range(ahead):
        for cp in loads(i):
            cp.start()
    for i in range(len(jobs)):
        for cp in loads(i):
            cp.wait()
        if i + ahead < len(jobs):
            for cp in loads(i + ahead):
                cp.start()
        compute(i)
        if i == 0:
            pl.semaphore_wait(barrier, tp_count + has_up.astype(jnp.int32) + has_down.astype(jnp.int32))
        else:
            send(i - 1)
    send(len(jobs) - 1)

    @pl.loop(parts, units)
    def _(unit):
        arrived(z, unit)
        here = place(z, core, unit)

        @pl.when(has_up)
        def _():
            going_up(here, here, z, unit).start()

        @pl.when(has_down)
        def _():
            going_down(here, here, z, unit).start()

        going_side(here, here, z, unit).start()

    early = units - late

    def set_aside(here, unit):
        part = pl.ds(pl.multiple_of((unit - early) * part_rows, part_rows), part_rows)
        return pltpu.make_async_copy(here, late_ref.at[part, :], late_sem.at[unit - early])

    @pl.loop(0, (planes - 1) * units - late)
    def _(m):
        distance, unit = m // units + 1, m % units
        below, above = z - distance, z + distance
        keeps = (distance == planes - 2) & (unit >= early)

        @pl.when(below >= 0)
        def _():
            arrived(below, unit)
            here = place(below, core, unit)

            @pl.when(has_up & jnp.logical_not(keeps))
            def _():
                going_up(here, here, below, unit).start()

            @pl.when(has_up & keeps)
            def _():
                set_aside(here, unit).start()

            going_side(here, here, below, unit).start()

        @pl.when(above < planes)
        def _():
            arrived(above, unit)
            here = place(above, core, unit)

            @pl.when(has_down & jnp.logical_not(keeps))
            def _():
                going_down(here, here, above, unit).start()

            @pl.when(has_down & keeps)
            def _():
                set_aside(here, unit).start()

            going_side(here, here, above, unit).start()

    for h in range(parts):
        keep(h).wait()
    for j in range(1, tp_count):
        for h in range(parts):
            flat_copy(j, h).wait_send()

    @pl.loop(0, planes * units)
    def _(m):
        plane, unit = m // units, m % units
        here = place(plane, core, unit)
        there = place(plane, 1 - core, unit)

        last = unit >= early
        held_up = last & (plane == 0) & (z == planes - 2)
        held_down = last & (plane == planes - 1) & (z == 1)
        missing = last & ((plane == 0) & (z == planes - 1) | (plane == planes - 1) & (z == 0))

        @pl.when((plane <= z) & has_up & jnp.logical_not(held_up))
        def _():
            going_up(here, here, plane, unit).wait_send()

        @pl.when((plane >= z) & has_down & jnp.logical_not(held_down))
        def _():
            going_down(here, here, plane, unit).wait_send()

        @pl.when(held_up | held_down)
        def _():
            set_aside(here, unit).wait()

        @pl.when(jnp.logical_not(missing))
        def _():
            going_side(here, here, plane, unit).wait_send()
            copy(there, there, side_send.at[plane, unit], side_recv.at[plane, unit], side).wait_recv()


def late_of(tp_count, rows):
    return min(3, tp_count * parts_of(rows) - 1)


def spread(dp_count, tp_count, *arrays):
    rows, cols = arrays[0].shape
    width = cols // tp_count
    parts = parts_of(rows)
    planes, units = dp_count // CORES, tp_count * parts
    grid = pltpu.SemaphoreType.DMA((planes, units))
    jobs = len(jobs_of(tp_count, rows))
    late = late_of(tp_count, rows)
    return pl.pallas_call(
        functools.partial(spread_kernel, dp_count, tp_count, parts, late),
        in_specs=[pl.BlockSpec(memory_space=pltpu.HBM)] * 4,
        out_specs=[pl.BlockSpec(memory_space=pl.ANY)] * 2,
        out_shape=[
            pltpu.VMEM((dp_count * tp_count * rows, width), jnp.bfloat16),
            pltpu.VMEM((late * rows // parts, width), jnp.bfloat16),
        ],
        scratch_shapes=[
            pltpu.VMEM((tp_count, 4, rows, width), jnp.float32),
            pltpu.VMEM((tp_count, rows, width), jnp.bfloat16),
            pltpu.SemaphoreType.DMA((jobs * 12,)),
            pltpu.SemaphoreType.DMA((parts,)),
            pltpu.SemaphoreType.DMA((late,)),
            pltpu.SemaphoreType.DMA((units,)),
        ]
        + [grid] * 5,
        compiler_params=pltpu.CompilerParams(collective_id=0, has_side_effects=True, vmem_limit_bytes=28 * 2**20),
        cost_estimate=pl.CostEstimate(flops=20 * rows * cols, bytes_accessed=16 * rows * cols, transcendentals=rows * cols),
    )(*[pltpu.with_memory_space_constraint(x, pltpu.HBM) for x in arrays])


def step_kernel(m_ref, g_ref, a_ref, s_ref, all_ref, nm_ref, na_ref, ns_ref, engine_ref, sems):
    count = sems.shape[0]
    rows = engine_ref.shape[0] // count

    def whole(n):
        part = pl.ds(n * rows, rows)
        return pltpu.make_async_copy(all_ref.at[part, :], engine_ref.at[part, :], sems.at[n])

    @pl.when(pl.program_id(0) == 0)
    def _():
        for n in range(count):
            whole(n).start()

    new_master, new_avg, new_avg_sq = step_math(m_ref[...], g_ref[...], a_ref[...], s_ref[...])
    nm_ref[...] = new_master
    na_ref[...] = new_avg
    ns_ref[...] = new_avg_sq

    @pl.when(pl.program_id(0) == pl.num_programs(0) - 1)
    def _():
        for n in range(count):
            whole(n).wait()


def local_step(arrays, gathered):
    rows, cols = arrays[0].shape
    tile = 16
    flat = pl.BlockSpec((tile, cols), lambda i: (i, 0))
    f32 = jax.ShapeDtypeStruct((rows, cols), jnp.float32)
    return pl.pallas_call(
        step_kernel,
        grid=(rows // tile,),
        in_specs=[flat] * 4 + [pl.BlockSpec(memory_space=pl.ANY)],
        out_specs=[flat] * 3 + [pl.BlockSpec(memory_space=pltpu.HBM)],
        out_shape=[f32] * 3 + [jax.ShapeDtypeStruct(gathered.shape, gathered.dtype)],
        scratch_shapes=[pltpu.SemaphoreType.DMA((4,))],
        compiler_params=pltpu.CompilerParams(vmem_limit_bytes=24 * 2**20),
        cost_estimate=pl.CostEstimate(
            flops=20 * rows * cols,
            bytes_accessed=28 * rows * cols + 2 * gathered.size,
            transcendentals=rows * cols,
        ),
    )(*[pltpu.with_memory_space_constraint(x, pltpu.HBM) for x in arrays], pltpu.with_memory_space_constraint(gathered, pltpu.VMEM))


def exchange_kernel(late_ref, other_ref, send_sem, recv_sem):
    dp = lax.axis_index("dp")
    side = {"dp": dp // CORES * CORES + 1 - dp % CORES}
    barrier = pltpu.get_barrier_semaphore()
    pl.semaphore_signal(barrier, inc=1, device_id=side, device_id_type=MESH)
    pl.semaphore_wait(barrier, 1)
    cp = pltpu.make_async_remote_copy(
        src_ref=late_ref, dst_ref=other_ref, send_sem=send_sem, recv_sem=recv_sem, device_id=side, device_id_type=MESH
    )
    cp.start()
    cp.wait()


def exchange(arrived):
    return pl.pallas_call(
        exchange_kernel,
        in_specs=[pl.BlockSpec(memory_space=pl.ANY)],
        out_specs=pl.BlockSpec(memory_space=pl.ANY),
        out_shape=pltpu.VMEM(arrived.shape, arrived.dtype),
        scratch_shapes=[pltpu.SemaphoreType.DMA, pltpu.SemaphoreType.DMA],
        compiler_params=pltpu.CompilerParams(collective_id=1, has_side_effects=True, vmem_limit_bytes=2**20),
        cost_estimate=pl.CostEstimate(flops=1, bytes_accessed=4 * arrived.size, transcendentals=0),
    )(pltpu.with_memory_space_constraint(arrived, pltpu.VMEM))


def store_kernel(dp_count, tp_count, rows, _, late_ref, other_ref, engine_ref, sems):
    planes, parts = dp_count // CORES, parts_of(rows)
    part_rows = rows // parts
    late = late_ref.shape[0] // part_rows
    early = tp_count * parts - late
    dp, t = lax.axis_index("dp"), lax.axis_index("tp")
    z, core = dp // CORES, dp % CORES

    @pl.when((z == 0) | (z == planes - 1))
    def _():
        plane = planes - 1 - z
        copies = []
        for which, (ref, owner) in enumerate([(late_ref, core), (other_ref, 1 - core)]):
            for n in range(late):
                unit = early + n
                block = (plane * CORES + owner) * tp_count + mix(t, unit // parts, tp_count)
                start = pl.multiple_of(block * rows + unit % parts * part_rows, part_rows)
                copies.append(
                    pltpu.make_async_copy(
                        ref.at[pl.ds(n * part_rows, part_rows), :],
                        engine_ref.at[pl.ds(start, part_rows), :],
                        sems.at[which * late + n],
                    )
                )
        for cp in copies:
            cp.start()
        for cp in copies:
            cp.wait()


def store(dp_count, tp_count, rows, engine, arrived, other):
    late = late_of(tp_count, rows)
    return pl.pallas_call(
        functools.partial(store_kernel, dp_count, tp_count, rows),
        in_specs=[pl.BlockSpec(memory_space=pltpu.HBM)] + [pl.BlockSpec(memory_space=pl.ANY)] * 2,
        out_specs=pl.BlockSpec(memory_space=pltpu.HBM),
        out_shape=jax.ShapeDtypeStruct(engine.shape, engine.dtype),
        input_output_aliases={0: 0},
        scratch_shapes=[pltpu.SemaphoreType.DMA((2 * late,))],
        compiler_params=pltpu.CompilerParams(vmem_limit_bytes=2**20),
        cost_estimate=pl.CostEstimate(flops=1, bytes_accessed=8 * arrived.size, transcendentals=0),
    )(engine, *[pltpu.with_memory_space_constraint(x, pltpu.VMEM) for x in (arrived, other)])


def body(dp_count, tp_count, *arrays):
    gathered, late = spread(dp_count, tp_count, *arrays)
    top = dp_count - CORES
    pairs = [(top - CORES + c, top + c) for c in range(CORES)] + [(CORES + c, c) for c in range(CORES)]
    arrived = lax.ppermute(late, "dp", pairs)
    new_master, new_avg, new_avg_sq, engine = local_step(arrays, gathered)
    engine = store(dp_count, tp_count, arrays[0].shape[0], engine, arrived, exchange(arrived))
    return new_master, new_avg, new_avg_sq, engine


def solution(mesh):
    flat = P(("dp", "tp"), None)
    return jax.shard_map(
        functools.partial(body, mesh.shape["dp"], mesh.shape["tp"]),
        mesh=mesh,
        in_specs=(flat,) * 4,
        out_specs=(flat, flat, flat, P(None, "tp")),
        check_vma=False,
    )
```

```python
import functools

import jax
import jax.numpy as jnp
from jax import lax
from jax.experimental import pallas as pl
from jax.experimental.pallas import tpu as pltpu
from jax.sharding import PartitionSpec as P

QH = 64
KVH = 8
HS = 128
CORES = 2
STEP = 16
LAG = 2
TAIL = (1, 1)
MESH = pl.DeviceIdType.MESH


def step_math(master, grad, exp_avg, exp_avg_sq):
    corr_one = 1.0 - 0.9**10
    corr_two = 1.0 - 0.999**10
    new_avg = 0.9 * exp_avg + 0.1 * grad
    new_avg_sq = 0.999 * exp_avg_sq + 0.001 * grad * grad
    update = new_avg / corr_one / (jnp.sqrt(new_avg_sq / corr_two) + 1e-08)
    new_master = master - 0.001 * (update + 0.1 * master)
    return new_master, new_avg, new_avg_sq


def pieces_of(tp_count, t):
    q, kv = QH // tp_count * HS, KVH // tp_count * HS
    return [(t * q, q, 0), (QH * HS + t * kv, kv, q), ((QH + KVH) * HS + t * kv, kv, q + kv)]


def mix(t, j, count):
    out, bit = 0, 1
    while bit < count:
        out = out + ((t // bit) % 2 + (j // bit) % 2) % 2 * bit
        bit *= 2
    return out


def parts_of(rows):
    return 2 if rows % 64 == 0 else 1


def jobs_of(tp_count, rows):
    part_rows = rows // parts_of(rows)
    jobs, start = [], 0
    first = [STEP, STEP]
    while sum(first) < part_rows:
        first.append(min(sum(first), part_rows - sum(first)))
    for size in first + [part_rows] * (rows // part_rows - 1):
        jobs.append((0, start, size))
        start += size
    for j in range(1, tp_count):
        for h in range(rows // part_rows):
            jobs.append((j, h * part_rows, part_rows))
    return jobs


def spread_kernel(dp_count, tp_count, parts, *refs):
    count = 5 + len(late_pieces(tp_count, refs[0].shape[0]))
    sources, (out_ref, *late_refs), (held, mine, load_sem) = refs[:4], refs[4:count], refs[count : count + 3]
    own_sem, late_sem, given_sem, flat_send, up_send, down_send, side_send, in_recv, side_recv = refs[count + 3 :]
    planes = dp_count // CORES
    dp, t = lax.axis_index("dp"), lax.axis_index("tp")
    z, core = dp // CORES, dp % CORES
    rows = mine.shape[1]
    part_rows = rows // parts
    has_up, has_down = z < planes - 1, z > 0
    units = tp_count * parts

    up = {"dp": dp + CORES}
    down = {"dp": dp - CORES}
    side = {"dp": z * CORES + 1 - core}

    barrier = pltpu.get_barrier_semaphore()
    for j in range(1, tp_count):
        pl.semaphore_signal(barrier, inc=1, device_id={"tp": mix(t, j, tp_count)}, device_id_type=MESH)
    pl.semaphore_signal(barrier, inc=1, device_id=side, device_id_type=MESH)

    @pl.when(has_up)
    def _():
        pl.semaphore_signal(barrier, inc=1, device_id=up, device_id_type=MESH)

    @pl.when(has_down)
    def _():
        pl.semaphore_signal(barrier, inc=1, device_id=down, device_id_type=MESH)

    jobs = jobs_of(tp_count, rows)

    def loads(i):
        j, first, size = jobs[i]
        part = pl.ds(first, size)
        return [
            pltpu.make_async_copy(
                sources[n].at[part, pl.ds(pl.multiple_of(start, HS), width)],
                held.at[j, n, part, pl.ds(into, width)],
                load_sem.at[(i * 4 + n) * 3 + k],
            )
            for n in range(4)
            for k, (start, width, into) in enumerate(pieces_of(tp_count, mix(t, j, tp_count)))
        ]

    def compute(i):
        j, first, size = jobs[i]

        def rows_at(start):
            part = pl.ds(start, STEP)
            new_master = step_math(*[held[j, n, part, :] for n in range(4)])[0]
            mine[j, part, :] = new_master.astype(jnp.bfloat16)

        if size == STEP:
            rows_at(first)
        else:

            @pl.loop(0, size // STEP)
            def _(k):
                rows_at(pl.multiple_of(first + k * STEP, STEP))

    def place(plane, which_core, unit):
        source = mix(t, unit // parts, tp_count)
        block = (plane * CORES + which_core) * tp_count + source
        start = block * rows + unit % parts * part_rows
        return out_ref.at[pl.ds(pl.multiple_of(start, part_rows), part_rows), :]

    def copy(src, dst, send, recv, target):
        return pltpu.make_async_remote_copy(
            src_ref=src, dst_ref=dst, send_sem=send, recv_sem=recv, device_id=target, device_id_type=MESH
        )

    def going_up(src, dst, plane, unit):
        return copy(src, dst, up_send.at[plane, unit], in_recv.at[plane, unit], up)

    def going_down(src, dst, plane, unit):
        return copy(src, dst, down_send.at[plane, unit], in_recv.at[plane, unit], down)

    def going_side(src, dst, plane, unit):
        return copy(src, dst, side_send.at[plane, unit], side_recv.at[plane, unit], side)

    def arrived(plane, unit):
        here = place(plane, core, unit)
        copy(here, here, side_send.at[plane, unit], in_recv.at[plane, unit], side).wait_recv()

    def home(first, size):
        start = ((z * CORES + core) * tp_count + t) * rows + first
        return out_ref.at[pl.ds(pl.multiple_of(start, STEP), size), :]

    def flat_copy(j, h):
        part = pl.ds(h * part_rows, part_rows)
        unit = j * parts + h
        target = {"tp": mix(t, j, tp_count)}
        return copy(mine.at[j, part, :], home(h * part_rows, part_rows), flat_send.at[unit], in_recv.at[z, unit], target)

    def keep(h):
        return pltpu.make_async_copy(mine.at[0, pl.ds(h * part_rows, part_rows), :], place(z, core, h), own_sem.at[h])

    def send(i):
        j, first, size = jobs[i]
        h = first // part_rows
        if j > 0:
            flat_copy(j, h).start()
            return
        src, dst = mine.at[0, pl.ds(first, size), :], home(first, size)

        @pl.when(has_up)
        def _():
            going_up(src, dst, z, h).start()

        @pl.when(has_down)
        def _():
            going_down(src, dst, z, h).start()

        going_side(src, dst, z, h).start()
        if (first + size) % part_rows == 0:
            keep(h).start()

    ahead = 2
    for i in range(ahead):
        for cp in loads(i):
            cp.start()
    for i in range(len(jobs)):
        for cp in loads(i):
            cp.wait()
        if i + ahead < len(jobs):
            for cp in loads(i + ahead):
                cp.start()
        compute(i)
        if i == 0:
            pl.semaphore_wait(barrier, tp_count + has_up.astype(jnp.int32) + has_down.astype(jnp.int32))
        else:
            send(i - 1)
    send(len(jobs) - 1)

    @pl.loop(parts, units)
    def _(unit):
        arrived(z, unit)
        here = place(z, core, unit)

        @pl.when(has_up)
        def _():
            going_up(here, here, z, unit).start()

        @pl.when(has_down)
        def _():
            going_down(here, here, z, unit).start()

        going_side(here, here, z, unit).start()

    def sides_done(plane, unit):
        here, there = place(plane, core, unit), place(plane, 1 - core, unit)
        going_side(here, here, plane, unit).wait_send()
        copy(there, there, side_send.at[plane, unit], side_recv.at[plane, unit], side).wait_recv()

    def settle(m):
        distance, unit = m // units, m % units
        below, above = z - distance, z + distance

        @pl.when(below >= 0)
        def _():
            sides_done(below, unit)

        @pl.when((above < planes) & (distance > 0))
        def _():
            sides_done(above, unit)

    both, late, given = shares_of(tp_count, rows)
    alone = units - late
    total = (planes - 1) * units + both
    first = jnp.where(core == 0, both, alone)
    low, high = z == 1, z == planes - 2

    def own_sent():
        for h in range(parts):
            keep(h).wait()
        for j in range(1, tp_count):
            for h in range(parts):
                flat_copy(j, h).wait_send()

        @pl.loop(0, units - LAG)
        def _(unit):
            settle(unit)

        @pl.loop(0, units)
        def _(unit):
            here = place(z, core, unit)

            @pl.when(has_up)
            def _():
                going_up(here, here, z, unit).wait_send()

            @pl.when(has_down)
            def _():
                going_down(here, here, z, unit).wait_send()

    def set_aside(here, which, n):
        part = pl.ds(pl.multiple_of(n * part_rows, part_rows), part_rows)
        return pltpu.make_async_copy(here, late_refs[which].at[part, :], late_sem.at[which, n])

    def set_aside_start(here, n):
        for which, (skip, size) in enumerate(late_pieces(tp_count, rows)):

            @pl.when((n >= skip) & (n < skip + size))
            def _():
                set_aside(here, which, n - skip).start()

    def hand_over(plane, n, target):
        here = place(plane, 0, units - given + n)
        return copy(here, here, given_sem.at[0, n], given_sem.at[1, n], target)

    @pl.loop(units, total)
    def _(m):
        distance, unit = m // units, m % units
        below, above = z - distance, z + distance
        keeps = (distance == planes - 2) & (unit >= first)
        aside = keeps & (unit < first + late)

        @pl.when(below >= 0)
        def _():
            arrived(below, unit)
            here = place(below, core, unit)

            @pl.when(has_up & jnp.logical_not(keeps))
            def _():
                going_up(here, here, below, unit).start()

            @pl.when(has_up & aside)
            def _():
                set_aside_start(here, unit - first)

            going_side(here, here, below, unit).start()

        @pl.when(above < planes)
        def _():
            arrived(above, unit)
            here = place(above, core, unit)

            @pl.when(has_down & jnp.logical_not(keeps))
            def _():
                going_down(here, here, above, unit).start()

            @pl.when(has_down & aside)
            def _():
                set_aside_start(here, unit - first)

            going_side(here, here, above, unit).start()

        settle(m - LAG)

        @pl.when(m == (planes - 1) * units)
        def _():
            own_sent()

        given_m = m - LAG - ((planes - 1) * units - given)

        @pl.when((given_m >= 0) & (given_m < given) & (core == 1))
        def _():
            @pl.when(high)
            def _():
                hand_over(0, given_m, up).start()

            @pl.when(low)
            def _():
                hand_over(planes - 1, given_m, down).start()

    @pl.loop(total - LAG, total)
    def _(m):
        settle(m)

    @pl.when(core == 1)
    def _():
        for plane, ends, starts, target in ((0, z == planes - 1, high, up), (planes - 1, z == 0, low, down)):

            @pl.when(ends)
            def _():
                @pl.loop(both, alone)
                def _(unit):
                    arrived(plane, unit)

                for n in range(given):
                    hand_over(plane, n, side).wait_recv()

            @pl.when(starts)
            def _():
                for n in range(given):
                    hand_over(plane, n, target).wait_send()

    @pl.when(low | high)
    def _():
        for which, (_, size) in enumerate(late_pieces(tp_count, rows)):
            for n in range(size):
                set_aside(late_refs[which].at[pl.ds(0, part_rows), :], which, n).wait()

    @pl.loop(0, jnp.where(has_up, z, 0) * units)
    def _(m):
        plane, unit = m // units, m % units
        here = place(plane, core, unit)

        @pl.when(jnp.logical_not((unit >= first) & (plane == 0) & high))
        def _():
            going_up(here, here, plane, unit).wait_send()

    @pl.loop((z + 1) * units, jnp.where(has_down, planes, z + 1) * units)
    def _(m):
        plane, unit = m // units, m % units
        here = place(plane, core, unit)

        @pl.when(jnp.logical_not((unit >= first) & (plane == planes - 1) & low))
        def _():
            going_down(here, here, plane, unit).wait_send()


def shares_of(tp_count, rows):
    units = tp_count * parts_of(rows)
    late, given = units // 2 + 1, 1
    return units - late - given, late, given


def late_pieces(tp_count, rows):
    late = shares_of(tp_count, rows)[1]
    sizes = (late - sum(TAIL),) + TAIL
    return [(sum(sizes[:i]), size) for i, size in enumerate(sizes)]


def spread(dp_count, tp_count, *arrays):
    rows, cols = arrays[0].shape
    width = cols // tp_count
    parts = parts_of(rows)
    planes, units = dp_count // CORES, tp_count * parts
    grid = pltpu.SemaphoreType.DMA((planes, units))
    jobs = len(jobs_of(tp_count, rows))
    late, pieces = shares_of(tp_count, rows)[1], late_pieces(tp_count, rows)
    return pl.pallas_call(
        functools.partial(spread_kernel, dp_count, tp_count, parts),
        in_specs=[pl.BlockSpec(memory_space=pltpu.HBM)] * 4,
        out_specs=[pl.BlockSpec(memory_space=pl.ANY)] * (1 + len(pieces)),
        out_shape=[
            pltpu.VMEM((dp_count * tp_count * rows, width), jnp.bfloat16),
        ]
        + [pltpu.VMEM((n * rows // parts, width), jnp.bfloat16) for _, n in pieces],
        scratch_shapes=[
            pltpu.VMEM((tp_count, 4, rows, width), jnp.float32),
            pltpu.VMEM((tp_count, rows, width), jnp.bfloat16),
            pltpu.SemaphoreType.DMA((jobs * 12,)),
            pltpu.SemaphoreType.DMA((parts,)),
            pltpu.SemaphoreType.DMA((len(pieces), late)),
            pltpu.SemaphoreType.DMA((2, shares_of(tp_count, rows)[2])),
            pltpu.SemaphoreType.DMA((units,)),
        ]
        + [grid] * 5,
        compiler_params=pltpu.CompilerParams(collective_id=0, has_side_effects=True, vmem_limit_bytes=28 * 2**20),
        cost_estimate=pl.CostEstimate(flops=20 * rows * cols, bytes_accessed=16 * rows * cols, transcendentals=rows * cols),
    )(*[pltpu.with_memory_space_constraint(x, pltpu.HBM) for x in arrays])


def step_kernel(m_ref, g_ref, a_ref, s_ref, all_ref, nm_ref, na_ref, ns_ref, engine_ref, sems):
    count = sems.shape[0]
    rows = engine_ref.shape[0] // count

    def whole(n):
        part = pl.ds(n * rows, rows)
        return pltpu.make_async_copy(all_ref.at[part, :], engine_ref.at[part, :], sems.at[n])

    @pl.when(pl.program_id(0) == 0)
    def _():
        for n in range(count):
            whole(n).start()

    new_master, new_avg, new_avg_sq = step_math(m_ref[...], g_ref[...], a_ref[...], s_ref[...])
    nm_ref[...] = new_master
    na_ref[...] = new_avg
    ns_ref[...] = new_avg_sq

    @pl.when(pl.program_id(0) == pl.num_programs(0) - 1)
    def _():
        for n in range(count):
            whole(n).wait()


def local_step(arrays, gathered):
    rows, cols = arrays[0].shape
    tile = 16
    flat = pl.BlockSpec((tile, cols), lambda i: (i, 0))
    f32 = jax.ShapeDtypeStruct((rows, cols), jnp.float32)
    return pl.pallas_call(
        step_kernel,
        grid=(rows // tile,),
        in_specs=[flat] * 4 + [pl.BlockSpec(memory_space=pl.ANY)],
        out_specs=[flat] * 3 + [pl.BlockSpec(memory_space=pltpu.HBM)],
        out_shape=[f32] * 3 + [jax.ShapeDtypeStruct(gathered.shape, gathered.dtype)],
        scratch_shapes=[pltpu.SemaphoreType.DMA((4,))],
        compiler_params=pltpu.CompilerParams(vmem_limit_bytes=24 * 2**20),
        cost_estimate=pl.CostEstimate(
            flops=20 * rows * cols,
            bytes_accessed=28 * rows * cols + 2 * gathered.size,
            transcendentals=rows * cols,
        ),
    )(*[pltpu.with_memory_space_constraint(x, pltpu.HBM) for x in arrays], pltpu.with_memory_space_constraint(gathered, pltpu.VMEM))


def far_unit(dp_count, tp_count, rows, ref, owner, unit):
    planes, parts = dp_count // CORES, parts_of(rows)
    part_rows = rows // parts
    z, t = lax.axis_index("dp") // CORES, lax.axis_index("tp")
    block = ((planes - 1 - z) * CORES + owner) * tp_count + mix(t, unit // parts, tp_count)
    start = block * rows + unit % parts * part_rows
    return ref.at[pl.ds(pl.multiple_of(start, part_rows), part_rows), :]


def unshared_of(tp_count, rows):
    both, late, given = shares_of(tp_count, rows)
    units = tp_count * parts_of(rows)
    return [(1, unit) for unit in range(both, units - late)] + [(0, unit) for unit in range(units - given, units)]


def greet(side):
    barrier = pltpu.get_barrier_semaphore()
    pl.semaphore_signal(barrier, inc=1, device_id=side, device_id_type=MESH)
    pl.semaphore_wait(barrier, 1)


def exchange_kernel(dp_count, tp_count, rows, *refs):
    planes, part_rows = dp_count // CORES, rows // parts_of(rows)
    dp = lax.axis_index("dp")
    z, core = dp // CORES, dp % CORES
    side = {"dp": z * CORES + 1 - core}
    greet(side)
    late_ref, other_ref, send_sems, recv_sems = refs[0], refs[-3], refs[-2], refs[-1]

    def copy(src, dst, n):
        return pltpu.make_async_remote_copy(
            src_ref=src,
            dst_ref=dst,
            send_sem=send_sems.at[n],
            recv_sem=recv_sems.at[n],
            device_id=side,
            device_id_type=MESH,
        )

    both_ways = copy(late_ref, other_ref, 0)
    missed = []
    if len(refs) > 4:
        all_ref, missed_ref = refs[1:3]
        for n, (owner, unit) in enumerate(unshared_of(tp_count, rows)):
            src = far_unit(dp_count, tp_count, rows, all_ref, owner, unit)
            missed.append(copy(src, missed_ref.at[pl.ds(n * part_rows, part_rows), :], n + 1))

    @pl.when((z == 0) | (z == planes - 1))
    def _():
        @pl.when(core == 1)
        def _():
            for cp in missed:
                cp.start()

        both_ways.start()

        @pl.when(core == 1)
        def _():
            for cp in missed:
                cp.wait_send()

        @pl.when(core == 0)
        def _():
            for cp in missed:
                cp.wait_recv()

        both_ways.wait()


def exchange(dp_count, tp_count, rows, number, arrived, *gathered):
    shapes = [arrived.shape]
    if gathered:
        shapes.insert(0, (len(unshared_of(tp_count, rows)) * rows // parts_of(rows), arrived.shape[1]))
    copies = 1 + len(unshared_of(tp_count, rows)) * len(gathered)
    return pl.pallas_call(
        functools.partial(exchange_kernel, dp_count, tp_count, rows),
        in_specs=[pl.BlockSpec(memory_space=pl.ANY)] * (1 + len(gathered)),
        out_specs=[pl.BlockSpec(memory_space=pl.ANY)] * len(shapes),
        out_shape=[pltpu.VMEM(shape, arrived.dtype) for shape in shapes],
        scratch_shapes=[pltpu.SemaphoreType.DMA((copies,))] * 2,
        compiler_params=pltpu.CompilerParams(collective_id=number, has_side_effects=True, vmem_limit_bytes=2**20),
        cost_estimate=pl.CostEstimate(flops=1, bytes_accessed=4 * arrived.size, transcendentals=0),
    )(*[pltpu.with_memory_space_constraint(x, pltpu.VMEM) for x in (arrived, *gathered)])


def store_kernel(dp_count, tp_count, rows, skip, _, late_ref, other_ref, *refs):
    engine_ref, sems = refs[-2:]
    planes, parts = dp_count // CORES, parts_of(rows)
    part_rows = rows // parts
    both, late, given = shares_of(tp_count, rows)
    alone = tp_count * parts - late
    dp = lax.axis_index("dp")
    z, core = dp // CORES, dp % CORES
    ends = (z == 0) | (z == planes - 1)

    def put(ref, n, owner, unit, sem):
        here = far_unit(dp_count, tp_count, rows, engine_ref, owner, unit)
        return pltpu.make_async_copy(ref.at[pl.ds(n * part_rows, part_rows), :], here, sems.at[sem])

    copies = []
    for ref, owner in ((late_ref, core), (other_ref, 1 - core)):
        for n in range(ref.shape[0] // part_rows):
            copies.append(put(ref, n, owner, n + skip + both + owner * (alone - both), len(copies)))
    missed = []
    if len(refs) > 2:
        missed = [put(refs[0], n, *u, len(copies) + n) for n, u in enumerate(unshared_of(tp_count, rows))]

    @pl.when(ends & (core == 0))
    def _():
        for cp in missed:
            cp.start()

    @pl.when(ends)
    def _():
        for cp in copies:
            cp.start()
        for cp in copies:
            cp.wait()

    @pl.when(ends & (core == 0))
    def _():
        for cp in missed:
            cp.wait()


def store(dp_count, tp_count, rows, skip, engine, *late):
    count = sum(x.shape[0] for x in late) * parts_of(rows) // rows
    return pl.pallas_call(
        functools.partial(store_kernel, dp_count, tp_count, rows, skip),
        in_specs=[pl.BlockSpec(memory_space=pltpu.HBM)] + [pl.BlockSpec(memory_space=pl.ANY)] * len(late),
        out_specs=pl.BlockSpec(memory_space=pltpu.HBM),
        out_shape=jax.ShapeDtypeStruct(engine.shape, engine.dtype),
        input_output_aliases={0: 0},
        scratch_shapes=[pltpu.SemaphoreType.DMA((count,))],
        compiler_params=pltpu.CompilerParams(vmem_limit_bytes=2**20),
        cost_estimate=pl.CostEstimate(flops=1, bytes_accessed=8 * late[0].size, transcendentals=0),
    )(engine, *[pltpu.with_memory_space_constraint(x, pltpu.VMEM) for x in late])


def body(dp_count, tp_count, *arrays):
    rows = arrays[0].shape[0]
    sizes = dp_count, tp_count, rows
    gathered, *late = spread(dp_count, tp_count, *arrays)
    top = dp_count - CORES
    pairs = [(top - CORES + c, top + c) for c in range(CORES)] + [(CORES + c, c) for c in range(CORES)]
    late = [lax.ppermute(x, "dp", pairs) for x in late]
    new_master, new_avg, new_avg_sq, engine = local_step(arrays, gathered)
    for n, (skip, _) in enumerate(late_pieces(tp_count, rows)):
        late[n], gathered, engine = lax.optimization_barrier((late[n], gathered, engine))
        *missed, other = exchange(*sizes, n + 1, late[n], *([gathered] if n == 0 else []))
        engine = store(*sizes, skip, engine, late[n], other, *missed)
    return new_master, new_avg, new_avg_sq, engine


def solution(mesh):
    flat = P(("dp", "tp"), None)
    return jax.shard_map(
        functools.partial(body, mesh.shape["dp"], mesh.shape["tp"]),
        mesh=mesh,
        in_specs=(flat,) * 4,
        out_specs=(flat, flat, flat, P(None, "tp")),
        check_vma=False,
    )
```

```python
import functools

import jax
import jax.numpy as jnp
from jax import lax
from jax.experimental import pallas as pl
from jax.experimental.pallas import tpu as pltpu
from jax.sharding import PartitionSpec as P

QH = 64
KVH = 8
HS = 128
CORES = 2
STEP = 16
AHEAD = 2
TAIL = (1, 1)
MESH = pl.DeviceIdType.MESH


def step_math(master, grad, exp_avg, exp_avg_sq):
    corr_one = 1.0 - 0.9**10
    corr_two = 1.0 - 0.999**10
    new_avg = 0.9 * exp_avg + 0.1 * grad
    new_avg_sq = 0.999 * exp_avg_sq + 0.001 * grad * grad
    update = new_avg / corr_one / (jnp.sqrt(new_avg_sq / corr_two) + 1e-08)
    new_master = master - 0.001 * (update + 0.1 * master)
    return new_master, new_avg, new_avg_sq


def pieces_of(tp_count, t):
    q, kv = QH // tp_count * HS, KVH // tp_count * HS
    return [(t * q, q, 0), (QH * HS + t * kv, kv, q), ((QH + KVH) * HS + t * kv, kv, q + kv)]


def mix(t, j, count):
    out, bit = 0, 1
    while bit < count:
        out = out + ((t // bit) % 2 + (j // bit) % 2) % 2 * bit
        bit *= 2
    return out


def parts_of(rows):
    return 2 if rows % 64 == 0 else 1


def jobs_of(tp_count, rows):
    part_rows = rows // parts_of(rows)
    jobs, start = [], 0
    first = [STEP, STEP]
    while sum(first) < part_rows:
        first.append(min(sum(first), part_rows - sum(first)))
    for size in first + [part_rows] * (rows // part_rows - 1):
        jobs.append((0, start, size))
        start += size
    for j in range(1, tp_count):
        for h in range(rows // part_rows):
            jobs.append((j, h * part_rows, part_rows))
    return jobs


def spread_kernel(dp_count, tp_count, parts, *refs):
    count = 5 + len(late_pieces(tp_count, refs[0].shape[0]))
    sources, (out_ref, *late_refs), (held, mine, load_sem) = refs[:4], refs[4:count], refs[count : count + 3]
    own_sem, late_sem, given_sem, flat_send, up_send, down_send, side_send, in_recv, side_recv = refs[count + 3 :]
    planes = dp_count // CORES
    dp, t = lax.axis_index("dp"), lax.axis_index("tp")
    z, core = dp // CORES, dp % CORES
    rows = mine.shape[1]
    part_rows = rows // parts
    has_up, has_down = z < planes - 1, z > 0
    units = tp_count * parts

    up = {"dp": dp + CORES}
    down = {"dp": dp - CORES}
    side = {"dp": z * CORES + 1 - core}

    barrier = pltpu.get_barrier_semaphore()
    for j in range(1, tp_count):
        pl.semaphore_signal(barrier, inc=1, device_id={"tp": mix(t, j, tp_count)}, device_id_type=MESH)
    pl.semaphore_signal(barrier, inc=1, device_id=side, device_id_type=MESH)

    @pl.when(has_up)
    def _():
        pl.semaphore_signal(barrier, inc=1, device_id=up, device_id_type=MESH)

    @pl.when(has_down)
    def _():
        pl.semaphore_signal(barrier, inc=1, device_id=down, device_id_type=MESH)

    jobs, ahead = jobs_of(tp_count, rows), AHEAD

    def loads(i):
        j, first, size = jobs[i]
        part = pl.ds(first, size)
        return [
            pltpu.make_async_copy(
                sources[n].at[part, pl.ds(pl.multiple_of(start, HS), width)],
                held.at[j, n, part, pl.ds(into, width)],
                load_sem.at[i % (ahead + 1)],
            )
            for n in range(4)
            for start, width, into in pieces_of(tp_count, mix(t, j, tp_count))
        ]

    def loaded(i):
        j, first, size = jobs[i]
        all_of_it = held.at[j, :, pl.ds(first, size), :]
        pltpu.make_async_copy(all_of_it, all_of_it, load_sem.at[i % (ahead + 1)]).wait()

    def compute(i):
        j, first, size = jobs[i]

        def rows_at(start):
            part = pl.ds(start, STEP)
            new_master = step_math(*[held[j, n, part, :] for n in range(4)])[0]
            mine[j, part, :] = new_master.astype(jnp.bfloat16)

        if size == STEP:
            rows_at(first)
        else:

            @pl.loop(0, size // STEP)
            def _(k):
                rows_at(pl.multiple_of(first + k * STEP, STEP))

    def place(plane, which_core, unit):
        source = mix(t, unit // parts, tp_count)
        block = (plane * CORES + which_core) * tp_count + source
        start = block * rows + unit % parts * part_rows
        return out_ref.at[pl.ds(pl.multiple_of(start, part_rows), part_rows), :]

    def copy(src, dst, send, recv, target):
        return pltpu.make_async_remote_copy(
            src_ref=src, dst_ref=dst, send_sem=send, recv_sem=recv, device_id=target, device_id_type=MESH
        )

    def going_up(src, dst, plane, unit):
        return copy(src, dst, up_send.at[plane], in_recv.at[plane, unit], up)

    def going_down(src, dst, plane, unit):
        return copy(src, dst, down_send.at[plane], in_recv.at[plane, unit], down)

    def going_side(src, dst, plane, unit):
        return copy(src, dst, side_send.at[plane], side_recv.at[plane], side)

    def arrived(plane, unit):
        here = place(plane, core, unit)
        copy(here, here, side_send.at[plane], in_recv.at[plane, unit], side).wait_recv()

    def home(first, size):
        start = ((z * CORES + core) * tp_count + t) * rows + first
        return out_ref.at[pl.ds(pl.multiple_of(start, STEP), size), :]

    def flat_copy(j, h):
        part = pl.ds(h * part_rows, part_rows)
        unit = j * parts + h
        target = {"tp": mix(t, j, tp_count)}
        return copy(mine.at[j, part, :], home(h * part_rows, part_rows), flat_send.at[0], in_recv.at[z, unit], target)

    def keep(h):
        return pltpu.make_async_copy(mine.at[0, pl.ds(h * part_rows, part_rows), :], place(z, core, h), own_sem.at[0])

    def send(i):
        j, first, size = jobs[i]
        h = first // part_rows
        if j > 0:
            flat_copy(j, h).start()
            return
        src, dst = mine.at[0, pl.ds(first, size), :], home(first, size)

        @pl.when(has_up)
        def _():
            going_up(src, dst, z, h).start()

        @pl.when(has_down)
        def _():
            going_down(src, dst, z, h).start()

        going_side(src, dst, z, h).start()
        if (first + size) % part_rows == 0:
            keep(h).start()

    for i in range(ahead):
        for cp in loads(i):
            cp.start()
    for i in range(len(jobs)):
        loaded(i)
        if i + ahead < len(jobs):
            for cp in loads(i + ahead):
                cp.start()
        compute(i)
        if i == 0:
            pl.semaphore_wait(barrier, tp_count + has_up.astype(jnp.int32) + has_down.astype(jnp.int32))
        else:
            send(i - 1)
    send(len(jobs) - 1)

    @pl.loop(parts, units)
    def _(unit):
        arrived(z, unit)
        here = place(z, core, unit)

        @pl.when(has_up)
        def _():
            going_up(here, here, z, unit).start()

        @pl.when(has_down)
        def _():
            going_down(here, here, z, unit).start()

        going_side(here, here, z, unit).start()

    both, late, given = shares_of(tp_count, rows)
    alone = units - late
    first = jnp.where(core == 0, both, alone)
    low, high = z == 1, z == planes - 2

    def sum_of(count, send_sem, recv_sem):
        here = out_ref.at[pl.ds(0, count * part_rows), :]
        return copy(here, here, send_sem, recv_sem, side)

    def sides_done(plane, count):
        done = sum_of(count, side_send.at[plane], side_recv.at[plane])
        done.wait_send()
        done.wait_recv()

    def set_aside(here, which, n):
        part = pl.ds(pl.multiple_of(n * part_rows, part_rows), part_rows)
        return pltpu.make_async_copy(here, late_refs[which].at[part, :], late_sem.at[which])

    def set_aside_start(here, n):
        for which, (skip, size) in enumerate(late_pieces(tp_count, rows)):

            @pl.when((n >= skip) & (n < skip + size))
            def _():
                set_aside(here, which, n - skip).start()

    def hand_over(plane, n, target):
        here = place(plane, 0, units - given + n)
        return copy(here, here, given_sem.at[0, n], given_sem.at[1, n], target)

    @pl.loop(units, (planes - 1) * units)
    def _(m):
        distance, unit = m // units, m % units
        below, above = z - distance, z + distance
        keeps = (distance == planes - 2) & (unit >= first)
        aside = keeps & (unit < first + late)

        @pl.when(below >= 0)
        def _():
            arrived(below, unit)
            here = place(below, core, unit)

            @pl.when(has_up & jnp.logical_not(keeps))
            def _():
                going_up(here, here, below, unit).start()

            @pl.when(has_up & aside)
            def _():
                set_aside_start(here, unit - first)

            going_side(here, here, below, unit).start()

        @pl.when(above < planes)
        def _():
            arrived(above, unit)
            here = place(above, core, unit)

            @pl.when(has_down & jnp.logical_not(keeps))
            def _():
                going_down(here, here, above, unit).start()

            @pl.when(has_down & aside)
            def _():
                set_aside_start(here, unit - first)

            going_side(here, here, above, unit).start()

    mine_all, flats = mine.at[0], mine.at[pl.ds(1, tp_count - 1)]
    pltpu.make_async_copy(mine_all, mine_all, own_sem.at[0]).wait()
    copy(flats, flats, flat_send.at[0], side_recv.at[z], side).wait_send()

    @pl.when(has_up)
    def _():
        sum_of(units, up_send.at[z], side_recv.at[z]).wait_send()

    @pl.when(has_down)
    def _():
        sum_of(units, down_send.at[z], side_recv.at[z]).wait_send()

    far = [((z == planes - 1), 0), ((z == 0), planes - 1)]

    @pl.loop(0, planes)
    def _(plane):
        @pl.when((plane - z < planes - 1) & (z - plane < planes - 1))
        def _():
            sides_done(plane, units)

    for starts, plane, target in ((high, 0, up), (low, planes - 1, down)):

        @pl.when(starts & (core == 1))
        def _():
            for n in range(given):
                hand_over(plane, n, target).start()

    for ends, plane in far:

        @pl.when(ends)
        def _():
            @pl.loop(0, both)
            def _(unit):
                arrived(plane, unit)
                here = place(plane, core, unit)
                going_side(here, here, plane, unit).start()

            sides_done(plane, both)

            @pl.when(core == 1)
            def _():
                @pl.loop(both, alone)
                def _(unit):
                    arrived(plane, unit)

                for n in range(given):
                    hand_over(plane, n, side).wait_recv()

    for starts, plane, target, sems in ((high, 0, up, up_send), (low, planes - 1, down, down_send)):

        @pl.when(starts)
        def _():
            for which, ref in enumerate(late_refs):
                pltpu.make_async_copy(ref, ref, late_sem.at[which]).wait()

            for owner, count in ((0, both), (1, alone)):

                @pl.when(core == owner)
                def _():
                    sum_of(count, sems.at[plane], side_recv.at[plane]).wait_send()
                    if owner == 1:
                        for n in range(given):
                            hand_over(plane, n, target).wait_send()

    @pl.loop(0, planes)
    def _(plane):
        @pl.when((plane < z) & has_up & jnp.logical_not((plane == 0) & high))
        def _():
            sum_of(units, up_send.at[plane], side_recv.at[plane]).wait_send()

        @pl.when((plane > z) & has_down & jnp.logical_not((plane == planes - 1) & low))
        def _():
            sum_of(units, down_send.at[plane], side_recv.at[plane]).wait_send()


def shares_of(tp_count, rows):
    units = tp_count * parts_of(rows)
    late, given = units // 2 + 1, 1
    return units - late - given, late, given


def late_pieces(tp_count, rows):
    late = shares_of(tp_count, rows)[1]
    sizes = (late - sum(TAIL),) + TAIL
    return [(sum(sizes[:i]), size) for i, size in enumerate(sizes)]


def spread(dp_count, tp_count, *arrays):
    rows, cols = arrays[0].shape
    width = cols // tp_count
    parts = parts_of(rows)
    planes, units = dp_count // CORES, tp_count * parts
    late, pieces = shares_of(tp_count, rows)[1], late_pieces(tp_count, rows)
    return pl.pallas_call(
        functools.partial(spread_kernel, dp_count, tp_count, parts),
        in_specs=[pl.BlockSpec(memory_space=pltpu.HBM)] * 4,
        out_specs=[pl.BlockSpec(memory_space=pl.ANY)] * (1 + len(pieces)),
        out_shape=[
            pltpu.VMEM((dp_count * tp_count * rows, width), jnp.bfloat16),
        ]
        + [pltpu.VMEM((n * rows // parts, width), jnp.bfloat16) for _, n in pieces],
        scratch_shapes=[
            pltpu.VMEM((tp_count, 4, rows, width), jnp.float32),
            pltpu.VMEM((tp_count, rows, width), jnp.bfloat16),
            pltpu.SemaphoreType.DMA((AHEAD + 1,)),
            pltpu.SemaphoreType.DMA((1,)),
            pltpu.SemaphoreType.DMA((len(pieces),)),
            pltpu.SemaphoreType.DMA((2, shares_of(tp_count, rows)[2])),
            pltpu.SemaphoreType.DMA((1,)),
            pltpu.SemaphoreType.DMA((planes,)),
            pltpu.SemaphoreType.DMA((planes,)),
            pltpu.SemaphoreType.DMA((planes,)),
            pltpu.SemaphoreType.DMA((planes, units)),
            pltpu.SemaphoreType.DMA((planes,)),
        ],
        compiler_params=pltpu.CompilerParams(collective_id=0, has_side_effects=True, vmem_limit_bytes=28 * 2**20),
        cost_estimate=pl.CostEstimate(flops=20 * rows * cols, bytes_accessed=16 * rows * cols, transcendentals=rows * cols),
    )(*[pltpu.with_memory_space_constraint(x, pltpu.HBM) for x in arrays])


def step_kernel(m_ref, g_ref, a_ref, s_ref, all_ref, nm_ref, na_ref, ns_ref, engine_ref, sems):
    count = sems.shape[0]
    rows = engine_ref.shape[0] // count

    def whole(n):
        part = pl.ds(n * rows, rows)
        return pltpu.make_async_copy(all_ref.at[part, :], engine_ref.at[part, :], sems.at[n])

    @pl.when(pl.program_id(0) == 0)
    def _():
        for n in range(count):
            whole(n).start()

    new_master, new_avg, new_avg_sq = step_math(m_ref[...], g_ref[...], a_ref[...], s_ref[...])
    nm_ref[...] = new_master
    na_ref[...] = new_avg
    ns_ref[...] = new_avg_sq

    @pl.when(pl.program_id(0) == pl.num_programs(0) - 1)
    def _():
        for n in range(count):
            whole(n).wait()


def local_step(arrays, gathered):
    rows, cols = arrays[0].shape
    tile = 16
    flat = pl.BlockSpec((tile, cols), lambda i: (i, 0))
    f32 = jax.ShapeDtypeStruct((rows, cols), jnp.float32)
    return pl.pallas_call(
        step_kernel,
        grid=(rows // tile,),
        in_specs=[flat] * 4 + [pl.BlockSpec(memory_space=pl.ANY)],
        out_specs=[flat] * 3 + [pl.BlockSpec(memory_space=pltpu.HBM)],
        out_shape=[f32] * 3 + [jax.ShapeDtypeStruct(gathered.shape, gathered.dtype)],
        scratch_shapes=[pltpu.SemaphoreType.DMA((4,))],
        compiler_params=pltpu.CompilerParams(vmem_limit_bytes=24 * 2**20),
        cost_estimate=pl.CostEstimate(
            flops=20 * rows * cols,
            bytes_accessed=28 * rows * cols + 2 * gathered.size,
            transcendentals=rows * cols,
        ),
    )(*[pltpu.with_memory_space_constraint(x, pltpu.HBM) for x in arrays], pltpu.with_memory_space_constraint(gathered, pltpu.VMEM))


def far_unit(dp_count, tp_count, rows, ref, owner, unit):
    planes, parts = dp_count // CORES, parts_of(rows)
    part_rows = rows // parts
    z, t = lax.axis_index("dp") // CORES, lax.axis_index("tp")
    block = ((planes - 1 - z) * CORES + owner) * tp_count + mix(t, unit // parts, tp_count)
    start = block * rows + unit % parts * part_rows
    return ref.at[pl.ds(pl.multiple_of(start, part_rows), part_rows), :]


def unshared_of(tp_count, rows):
    both, late, given = shares_of(tp_count, rows)
    units = tp_count * parts_of(rows)
    return [(1, unit) for unit in range(both, units - late)] + [(0, unit) for unit in range(units - given, units)]


def greet(side):
    barrier = pltpu.get_barrier_semaphore()
    pl.semaphore_signal(barrier, inc=1, device_id=side, device_id_type=MESH)
    pl.semaphore_wait(barrier, 1)


def exchange_kernel(dp_count, tp_count, rows, *refs):
    planes, part_rows = dp_count // CORES, rows // parts_of(rows)
    dp = lax.axis_index("dp")
    z, core = dp // CORES, dp % CORES
    side = {"dp": z * CORES + 1 - core}
    greet(side)
    late_ref, other_ref, send_sems, recv_sems = refs[0], refs[-3], refs[-2], refs[-1]

    def copy(src, dst, n):
        return pltpu.make_async_remote_copy(
            src_ref=src,
            dst_ref=dst,
            send_sem=send_sems.at[n],
            recv_sem=recv_sems.at[n],
            device_id=side,
            device_id_type=MESH,
        )

    both_ways = copy(late_ref, other_ref, 0)
    missed = []
    if len(refs) > 4:
        all_ref, missed_ref = refs[1:3]
        for n, (owner, unit) in enumerate(unshared_of(tp_count, rows)):
            src = far_unit(dp_count, tp_count, rows, all_ref, owner, unit)
            missed.append(copy(src, missed_ref.at[pl.ds(n * part_rows, part_rows), :], n + 1))

    @pl.when((z == 0) | (z == planes - 1))
    def _():
        @pl.when(core == 1)
        def _():
            for cp in missed:
                cp.start()

        both_ways.start()

        @pl.when(core == 1)
        def _():
            for cp in missed:
                cp.wait_send()

        @pl.when(core == 0)
        def _():
            for cp in missed:
                cp.wait_recv()

        both_ways.wait()


def exchange(dp_count, tp_count, rows, number, arrived, *gathered):
    shapes = [arrived.shape]
    if gathered:
        shapes.insert(0, (len(unshared_of(tp_count, rows)) * rows // parts_of(rows), arrived.shape[1]))
    copies = 1 + len(unshared_of(tp_count, rows)) * len(gathered)
    return pl.pallas_call(
        functools.partial(exchange_kernel, dp_count, tp_count, rows),
        in_specs=[pl.BlockSpec(memory_space=pl.ANY)] * (1 + len(gathered)),
        out_specs=[pl.BlockSpec(memory_space=pl.ANY)] * len(shapes),
        out_shape=[pltpu.VMEM(shape, arrived.dtype) for shape in shapes],
        scratch_shapes=[pltpu.SemaphoreType.DMA((copies,))] * 2,
        compiler_params=pltpu.CompilerParams(collective_id=number, has_side_effects=True, vmem_limit_bytes=2**20),
        cost_estimate=pl.CostEstimate(flops=1, bytes_accessed=4 * arrived.size, transcendentals=0),
    )(*[pltpu.with_memory_space_constraint(x, pltpu.VMEM) for x in (arrived, *gathered)])


def store_kernel(dp_count, tp_count, rows, skip, _, late_ref, other_ref, *refs):
    engine_ref, sems = refs[-2:]
    planes, parts = dp_count // CORES, parts_of(rows)
    part_rows = rows // parts
    both, late, given = shares_of(tp_count, rows)
    alone = tp_count * parts - late
    dp = lax.axis_index("dp")
    z, core = dp // CORES, dp % CORES
    ends = (z == 0) | (z == planes - 1)

    def put(ref, n, owner, unit, sem):
        here = far_unit(dp_count, tp_count, rows, engine_ref, owner, unit)
        return pltpu.make_async_copy(ref.at[pl.ds(n * part_rows, part_rows), :], here, sems.at[sem])

    copies = []
    for ref, owner in ((late_ref, core), (other_ref, 1 - core)):
        for n in range(ref.shape[0] // part_rows):
            copies.append(put(ref, n, owner, n + skip + both + owner * (alone - both), len(copies)))
    missed = []
    if len(refs) > 2:
        missed = [put(refs[0], n, *u, len(copies) + n) for n, u in enumerate(unshared_of(tp_count, rows))]

    @pl.when(ends & (core == 0))
    def _():
        for cp in missed:
            cp.start()

    @pl.when(ends)
    def _():
        for cp in copies:
            cp.start()
        for cp in copies:
            cp.wait()

    @pl.when(ends & (core == 0))
    def _():
        for cp in missed:
            cp.wait()


def store(dp_count, tp_count, rows, skip, engine, *late):
    count = sum(x.shape[0] for x in late) * parts_of(rows) // rows
    return pl.pallas_call(
        functools.partial(store_kernel, dp_count, tp_count, rows, skip),
        in_specs=[pl.BlockSpec(memory_space=pltpu.HBM)] + [pl.BlockSpec(memory_space=pl.ANY)] * len(late),
        out_specs=pl.BlockSpec(memory_space=pltpu.HBM),
        out_shape=jax.ShapeDtypeStruct(engine.shape, engine.dtype),
        input_output_aliases={0: 0},
        scratch_shapes=[pltpu.SemaphoreType.DMA((count,))],
        compiler_params=pltpu.CompilerParams(vmem_limit_bytes=2**20),
        cost_estimate=pl.CostEstimate(flops=1, bytes_accessed=8 * late[0].size, transcendentals=0),
    )(engine, *[pltpu.with_memory_space_constraint(x, pltpu.VMEM) for x in late])


def body(dp_count, tp_count, *arrays):
    rows = arrays[0].shape[0]
    sizes = dp_count, tp_count, rows
    gathered, *late = spread(dp_count, tp_count, *arrays)
    top = dp_count - CORES
    pairs = [(top - CORES + c, top + c) for c in range(CORES)] + [(CORES + c, c) for c in range(CORES)]
    late = [lax.ppermute(x, "dp", pairs) for x in late]
    new_master, new_avg, new_avg_sq, engine = local_step(arrays, gathered)
    for n, (skip, _) in enumerate(late_pieces(tp_count, rows)):
        late[n], gathered, engine = lax.optimization_barrier((late[n], gathered, engine))
        *missed, other = exchange(*sizes, n + 1, late[n], *([gathered] if n == 0 else []))
        engine = store(*sizes, skip, engine, late[n], other, *missed)
    return new_master, new_avg, new_avg_sq, engine


def solution(mesh):
    flat = P(("dp", "tp"), None)
    return jax.shard_map(
        functools.partial(body, mesh.shape["dp"], mesh.shape["tp"]),
        mesh=mesh,
        in_specs=(flat,) * 4,
        out_specs=(flat, flat, flat, P(None, "tp")),
        check_vma=False,
    )
```

```python
import functools

import jax
import jax.numpy as jnp
from jax import lax
from jax.experimental import pallas as pl
from jax.experimental.pallas import tpu as pltpu
from jax.sharding import PartitionSpec as P

QH = 64
KVH = 8
HS = 128
CORES = 2
STEP = 16
AHEAD = 2
TAIL = (1, 1)
UNSHARED = 1
MESH = pl.DeviceIdType.MESH


def step_math(master, grad, exp_avg, exp_avg_sq):
    corr_one = 1.0 - 0.9**10
    corr_two = 1.0 - 0.999**10
    new_avg = 0.9 * exp_avg + 0.1 * grad
    new_avg_sq = 0.999 * exp_avg_sq + 0.001 * grad * grad
    update = new_avg / corr_one / (jnp.sqrt(new_avg_sq / corr_two) + 1e-08)
    new_master = master - 0.001 * (update + 0.1 * master)
    return new_master, new_avg, new_avg_sq


def pieces_of(tp_count, t):
    q, kv = QH // tp_count * HS, KVH // tp_count * HS
    return [(t * q, q, 0), (QH * HS + t * kv, kv, q), ((QH + KVH) * HS + t * kv, kv, q + kv)]


def mix(t, j, count):
    out, bit = 0, 1
    while bit < count:
        out = out + ((t // bit) % 2 + (j // bit) % 2) % 2 * bit
        bit *= 2
    return out


def parts_of(rows):
    return 2 if rows % 64 == 0 else 1


def jobs_of(tp_count, rows):
    part_rows = rows // parts_of(rows)
    jobs, start = [], 0
    first = [STEP, STEP]
    while sum(first) < part_rows:
        first.append(min(sum(first), part_rows - sum(first)))
    for size in first + [part_rows] * (rows // part_rows - 1):
        jobs.append((0, start, size))
        start += size
    for j in range(1, tp_count):
        for h in range(rows // part_rows):
            jobs.append((j, h * part_rows, part_rows))
    return jobs


def spread_kernel(dp_count, tp_count, parts, *refs):
    count = 5 + len(late_pieces(tp_count, refs[0].shape[0]))
    sources, (out_ref, *late_refs), (held, mine, load_sem) = refs[:4], refs[4:count], refs[count : count + 3]
    own_sem, late_sem, given_sem, flat_send, up_send, down_send, side_send, in_recv, side_recv = refs[count + 3 :]
    planes = dp_count // CORES
    dp, t = lax.axis_index("dp"), lax.axis_index("tp")
    z, core = dp // CORES, dp % CORES
    rows = mine.shape[1]
    part_rows = rows // parts
    has_up, has_down = z < planes - 1, z > 0
    units = tp_count * parts

    up = {"dp": dp + CORES}
    down = {"dp": dp - CORES}
    side = {"dp": z * CORES + 1 - core}

    barrier = pltpu.get_barrier_semaphore()
    for j in reversed(range(1, tp_count)):
        pl.semaphore_signal(barrier, inc=1, device_id={"tp": mix(t, j, tp_count)}, device_id_type=MESH)
    pl.semaphore_signal(barrier, inc=1, device_id=side, device_id_type=MESH)

    @pl.when(has_up)
    def _():
        pl.semaphore_signal(barrier, inc=1, device_id=up, device_id_type=MESH)

    @pl.when(has_down)
    def _():
        pl.semaphore_signal(barrier, inc=1, device_id=down, device_id_type=MESH)

    jobs, ahead = jobs_of(tp_count, rows), AHEAD

    def loads(i):
        j, first, size = jobs[i]
        part = pl.ds(first, size)
        return [
            pltpu.make_async_copy(
                sources[n].at[part, pl.ds(pl.multiple_of(start, HS), width)],
                held.at[j, n, part, pl.ds(into, width)],
                load_sem.at[i % (ahead + 1)],
            )
            for n in range(4)
            for start, width, into in pieces_of(tp_count, mix(t, j, tp_count))
        ]

    def loaded(i):
        j, first, size = jobs[i]
        all_of_it = held.at[j, :, pl.ds(first, size), :]
        pltpu.make_async_copy(all_of_it, all_of_it, load_sem.at[i % (ahead + 1)]).wait()

    def compute(i):
        j, first, size = jobs[i]

        def rows_at(start):
            part = pl.ds(start, STEP)
            new_master = step_math(*[held[j, n, part, :] for n in range(4)])[0]
            mine[j, part, :] = new_master.astype(jnp.bfloat16)

        if size == STEP:
            rows_at(first)
        else:

            @pl.loop(0, size // STEP)
            def _(k):
                rows_at(pl.multiple_of(first + k * STEP, STEP))

    def place(plane, which_core, unit):
        source = mix(t, unit // parts, tp_count)
        block = (plane * CORES + which_core) * tp_count + source
        start = block * rows + unit % parts * part_rows
        return out_ref.at[pl.ds(pl.multiple_of(start, part_rows), part_rows), :]

    def copy(src, dst, send, recv, target):
        return pltpu.make_async_remote_copy(
            src_ref=src, dst_ref=dst, send_sem=send, recv_sem=recv, device_id=target, device_id_type=MESH
        )

    def going_up(src, dst, plane, unit):
        return copy(src, dst, up_send.at[plane], in_recv.at[plane, unit], up)

    def going_down(src, dst, plane, unit):
        return copy(src, dst, down_send.at[plane], in_recv.at[plane, unit], down)

    def going_side(src, dst, plane, unit):
        return copy(src, dst, side_send.at[plane], side_recv.at[plane], side)

    def arrived(plane, unit):
        here = place(plane, core, unit)
        copy(here, here, side_send.at[plane], in_recv.at[plane, unit], side).wait_recv()

    def home(first, size):
        start = ((z * CORES + core) * tp_count + t) * rows + first
        return out_ref.at[pl.ds(pl.multiple_of(start, STEP), size), :]

    def flat_copy(j, h):
        part = pl.ds(h * part_rows, part_rows)
        unit = j * parts + h
        target = {"tp": mix(t, j, tp_count)}
        return copy(mine.at[j, part, :], home(h * part_rows, part_rows), flat_send.at[0], in_recv.at[z, unit], target)

    def keep(h):
        return pltpu.make_async_copy(mine.at[0, pl.ds(h * part_rows, part_rows), :], place(z, core, h), own_sem.at[0])

    def send(i):
        j, first, size = jobs[i]
        h = first // part_rows
        if j > 0:
            flat_copy(j, h).start()
            return
        src, dst = mine.at[0, pl.ds(first, size), :], home(first, size)

        @pl.when(has_up)
        def _():
            going_up(src, dst, z, h).start()

        @pl.when(has_down)
        def _():
            going_down(src, dst, z, h).start()

        going_side(src, dst, z, h).start()
        if (first + size) % part_rows == 0:
            keep(h).start()

    for i in range(ahead):
        for cp in loads(i):
            cp.start()
    for i in range(len(jobs)):
        loaded(i)
        if i + ahead < len(jobs):
            for cp in loads(i + ahead):
                cp.start()
        compute(i)
        if i == 0:
            pl.semaphore_wait(barrier, tp_count + has_up.astype(jnp.int32) + has_down.astype(jnp.int32))
        else:
            send(i - 1)
    send(len(jobs) - 1)

    @pl.loop(parts, units)
    def _(unit):
        arrived(z, unit)
        here = place(z, core, unit)

        @pl.when(has_up)
        def _():
            going_up(here, here, z, unit).start()

        @pl.when(has_down)
        def _():
            going_down(here, here, z, unit).start()

        going_side(here, here, z, unit).start()

    both, late, given = shares_of(tp_count, rows)
    alone, shared = units - late, both - UNSHARED
    first = jnp.where(core == 0, both, alone)
    low, high = z == 1, z == planes - 2

    def sum_of(count, send_sem, recv_sem):
        here = out_ref.at[pl.ds(0, count * part_rows), :]
        return copy(here, here, send_sem, recv_sem, side)

    def sides_done(plane, count):
        done = sum_of(count, side_send.at[plane], side_recv.at[plane])
        done.wait_send()
        done.wait_recv()

    def set_aside(here, which, n):
        part = pl.ds(pl.multiple_of(n * part_rows, part_rows), part_rows)
        return pltpu.make_async_copy(here, late_refs[which].at[part, :], late_sem.at[which])

    def set_aside_start(here, n):
        for which, (skip, size) in enumerate(late_pieces(tp_count, rows)):

            @pl.when((n >= skip) & (n < skip + size))
            def _():
                set_aside(here, which, n - skip).start()

    def hand_over(plane, n, target):
        here = place(plane, 0, units - given + n)
        return copy(here, here, given_sem.at[0, n], given_sem.at[1, n], target)

    @pl.loop(units, (planes - 1) * units)
    def _(m):
        distance, unit = m // units, m % units
        below, above = z - distance, z + distance
        keeps = (distance == planes - 2) & (unit >= first)
        aside = keeps & (unit < first + late)

        @pl.when(below >= 0)
        def _():
            arrived(below, unit)
            here = place(below, core, unit)

            @pl.when(has_up & jnp.logical_not(keeps))
            def _():
                going_up(here, here, below, unit).start()

            @pl.when(has_up & aside)
            def _():
                set_aside_start(here, unit - first)

            going_side(here, here, below, unit).start()

        @pl.when(above < planes)
        def _():
            arrived(above, unit)
            here = place(above, core, unit)

            @pl.when(has_down & jnp.logical_not(keeps))
            def _():
                going_down(here, here, above, unit).start()

            @pl.when(has_down & aside)
            def _():
                set_aside_start(here, unit - first)

            going_side(here, here, above, unit).start()

    mine_all, flats = mine.at[0], mine.at[pl.ds(1, tp_count - 1)]
    pltpu.make_async_copy(mine_all, mine_all, own_sem.at[0]).wait()
    copy(flats, flats, flat_send.at[0], side_recv.at[z], side).wait_send()

    @pl.when(has_up)
    def _():
        sum_of(units, up_send.at[z], side_recv.at[z]).wait_send()

    @pl.when(has_down)
    def _():
        sum_of(units, down_send.at[z], side_recv.at[z]).wait_send()

    far = [((z == planes - 1), 0), ((z == 0), planes - 1)]

    @pl.loop(0, planes)
    def _(plane):
        @pl.when((plane - z < planes - 1) & (z - plane < planes - 1))
        def _():
            sides_done(plane, units)

    for starts, plane, target in ((high, 0, up), (low, planes - 1, down)):

        @pl.when(starts & (core == 1))
        def _():
            for n in range(given):
                hand_over(plane, n, target).start()

    for ends, plane in far:

        @pl.when(ends)
        def _():
            @pl.loop(0, shared)
            def _(unit):
                arrived(plane, unit)
                here = place(plane, core, unit)
                going_side(here, here, plane, unit).start()

            @pl.loop(shared, both)
            def _(unit):
                arrived(plane, unit)

            sides_done(plane, shared)

            @pl.when(core == 1)
            def _():
                @pl.loop(both, alone)
                def _(unit):
                    arrived(plane, unit)

                for n in range(given):
                    hand_over(plane, n, side).wait_recv()

    for starts, plane, target, sems in ((high, 0, up, up_send), (low, planes - 1, down, down_send)):

        @pl.when(starts)
        def _():
            for which, ref in enumerate(late_refs):
                pltpu.make_async_copy(ref, ref, late_sem.at[which]).wait()

            for owner, count in ((0, both), (1, alone)):

                @pl.when(core == owner)
                def _():
                    sum_of(count, sems.at[plane], side_recv.at[plane]).wait_send()
                    if owner == 1:
                        for n in range(given):
                            hand_over(plane, n, target).wait_send()

    @pl.loop(0, planes)
    def _(plane):
        @pl.when((plane < z) & has_up & jnp.logical_not((plane == 0) & high))
        def _():
            sum_of(units, up_send.at[plane], side_recv.at[plane]).wait_send()

        @pl.when((plane > z) & has_down & jnp.logical_not((plane == planes - 1) & low))
        def _():
            sum_of(units, down_send.at[plane], side_recv.at[plane]).wait_send()


def shares_of(tp_count, rows):
    units = tp_count * parts_of(rows)
    late, given = units // 2 + 1, 1
    return units - late - given, late, given


def late_pieces(tp_count, rows):
    late = shares_of(tp_count, rows)[1]
    sizes = (late - sum(TAIL),) + TAIL
    return [(sum(sizes[:i]), size) for i, size in enumerate(sizes)]


def spread(dp_count, tp_count, *arrays):
    rows, cols = arrays[0].shape
    width = cols // tp_count
    parts = parts_of(rows)
    planes, units = dp_count // CORES, tp_count * parts
    late, pieces = shares_of(tp_count, rows)[1], late_pieces(tp_count, rows)
    return pl.pallas_call(
        functools.partial(spread_kernel, dp_count, tp_count, parts),
        in_specs=[pl.BlockSpec(memory_space=pltpu.HBM)] * 4,
        out_specs=[pl.BlockSpec(memory_space=pl.ANY)] * (1 + len(pieces)),
        out_shape=[
            pltpu.VMEM((dp_count * tp_count * rows, width), jnp.bfloat16),
        ]
        + [pltpu.VMEM((n * rows // parts, width), jnp.bfloat16) for _, n in pieces],
        scratch_shapes=[
            pltpu.VMEM((tp_count, 4, rows, width), jnp.float32),
            pltpu.VMEM((tp_count, rows, width), jnp.bfloat16),
            pltpu.SemaphoreType.DMA((AHEAD + 1,)),
            pltpu.SemaphoreType.DMA((1,)),
            pltpu.SemaphoreType.DMA((len(pieces),)),
            pltpu.SemaphoreType.DMA((2, shares_of(tp_count, rows)[2])),
            pltpu.SemaphoreType.DMA((1,)),
            pltpu.SemaphoreType.DMA((planes,)),
            pltpu.SemaphoreType.DMA((planes,)),
            pltpu.SemaphoreType.DMA((planes,)),
            pltpu.SemaphoreType.DMA((planes, units)),
            pltpu.SemaphoreType.DMA((planes,)),
        ],
        compiler_params=pltpu.CompilerParams(collective_id=0, has_side_effects=True, vmem_limit_bytes=28 * 2**20),
        cost_estimate=pl.CostEstimate(flops=20 * rows * cols, bytes_accessed=16 * rows * cols, transcendentals=rows * cols),
    )(*[pltpu.with_memory_space_constraint(x, pltpu.HBM) for x in arrays])


def step_kernel(m_ref, g_ref, a_ref, s_ref, all_ref, nm_ref, na_ref, ns_ref, engine_ref, sems):
    count = sems.shape[0]
    rows = engine_ref.shape[0] // count

    def whole(n):
        part = pl.ds(n * rows, rows)
        return pltpu.make_async_copy(all_ref.at[part, :], engine_ref.at[part, :], sems.at[n])

    @pl.when(pl.program_id(0) == 0)
    def _():
        for n in range(count):
            whole(n).start()

    new_master, new_avg, new_avg_sq = step_math(m_ref[...], g_ref[...], a_ref[...], s_ref[...])
    nm_ref[...] = new_master
    na_ref[...] = new_avg
    ns_ref[...] = new_avg_sq

    @pl.when(pl.program_id(0) == pl.num_programs(0) - 1)
    def _():
        for n in range(count):
            whole(n).wait()


def local_step(arrays, gathered):
    rows, cols = arrays[0].shape
    tile = 16
    flat = pl.BlockSpec((tile, cols), lambda i: (i, 0))
    f32 = jax.ShapeDtypeStruct((rows, cols), jnp.float32)
    return pl.pallas_call(
        step_kernel,
        grid=(rows // tile,),
        in_specs=[flat] * 4 + [pl.BlockSpec(memory_space=pl.ANY)],
        out_specs=[flat] * 3 + [pl.BlockSpec(memory_space=pltpu.HBM)],
        out_shape=[f32] * 3 + [jax.ShapeDtypeStruct(gathered.shape, gathered.dtype)],
        scratch_shapes=[pltpu.SemaphoreType.DMA((4,))],
        compiler_params=pltpu.CompilerParams(vmem_limit_bytes=24 * 2**20),
        cost_estimate=pl.CostEstimate(
            flops=20 * rows * cols,
            bytes_accessed=28 * rows * cols + 2 * gathered.size,
            transcendentals=rows * cols,
        ),
    )(*[pltpu.with_memory_space_constraint(x, pltpu.HBM) for x in arrays], pltpu.with_memory_space_constraint(gathered, pltpu.VMEM))


def far_unit(dp_count, tp_count, rows, ref, owner, unit):
    planes, parts = dp_count // CORES, parts_of(rows)
    part_rows = rows // parts
    z, t = lax.axis_index("dp") // CORES, lax.axis_index("tp")
    block = ((planes - 1 - z) * CORES + owner) * tp_count + mix(t, unit // parts, tp_count)
    start = block * rows + unit % parts * part_rows
    return ref.at[pl.ds(pl.multiple_of(start, part_rows), part_rows), :]


def unshared_of(tp_count, rows, core):
    both, late, given = shares_of(tp_count, rows)
    units = tp_count * parts_of(rows)
    if core == 0:
        return [(0, unit) for unit in range(both - UNSHARED, both)]
    return [(1, unit) for unit in range(both - UNSHARED, units - late)] + [(0, unit) for unit in range(units - given, units)]


def greet(side):
    barrier = pltpu.get_barrier_semaphore()
    pl.semaphore_signal(barrier, inc=1, device_id=side, device_id_type=MESH)
    pl.semaphore_wait(barrier, 1)


def exchange_kernel(dp_count, tp_count, rows, *refs):
    planes, part_rows = dp_count // CORES, rows // parts_of(rows)
    dp = lax.axis_index("dp")
    z, core = dp // CORES, dp % CORES
    side = {"dp": z * CORES + 1 - core}
    greet(side)
    late_ref, other_ref, send_sems, recv_sems = refs[0], refs[-3], refs[-2], refs[-1]

    def copy(src, dst, n):
        return pltpu.make_async_remote_copy(
            src_ref=src,
            dst_ref=dst,
            send_sem=send_sems.at[n],
            recv_sem=recv_sems.at[n],
            device_id=side,
            device_id_type=MESH,
        )

    both_ways = copy(late_ref, other_ref, 0)
    missed = ([], [])
    if len(refs) > 4:
        all_ref, missed_ref = refs[1:3]
        for owner_core, copies in enumerate(missed):
            for n, (owner, unit) in enumerate(unshared_of(tp_count, rows, owner_core)):
                src = far_unit(dp_count, tp_count, rows, all_ref, owner, unit)
                copies.append(copy(src, missed_ref.at[pl.ds(n * part_rows, part_rows), :], n + 1))

    @pl.when((z == 0) | (z == planes - 1))
    def _():
        for mine in range(CORES):

            @pl.when(core == mine)
            def _():
                for cp in missed[mine]:
                    cp.start()
                both_ways.start()
                for cp in missed[mine]:
                    cp.wait_send()
                for cp in missed[1 - mine]:
                    cp.wait_recv()

        both_ways.wait()


def exchange(dp_count, tp_count, rows, number, arrived, *gathered):
    shapes = [arrived.shape]
    if gathered:
        shapes.insert(0, (len(unshared_of(tp_count, rows, 1)) * rows // parts_of(rows), arrived.shape[1]))
    copies = 1 + len(unshared_of(tp_count, rows, 1)) * len(gathered)
    return pl.pallas_call(
        functools.partial(exchange_kernel, dp_count, tp_count, rows),
        in_specs=[pl.BlockSpec(memory_space=pl.ANY)] * (1 + len(gathered)),
        out_specs=[pl.BlockSpec(memory_space=pl.ANY)] * len(shapes),
        out_shape=[pltpu.VMEM(shape, arrived.dtype) for shape in shapes],
        scratch_shapes=[pltpu.SemaphoreType.DMA((copies,))] * 2,
        compiler_params=pltpu.CompilerParams(collective_id=number, has_side_effects=True, vmem_limit_bytes=2**20),
        cost_estimate=pl.CostEstimate(flops=1, bytes_accessed=4 * arrived.size, transcendentals=0),
    )(*[pltpu.with_memory_space_constraint(x, pltpu.VMEM) for x in (arrived, *gathered)])


def store_kernel(dp_count, tp_count, rows, skip, _, late_ref, other_ref, *refs):
    engine_ref, sems = refs[-2:]
    planes, parts = dp_count // CORES, parts_of(rows)
    part_rows = rows // parts
    both, late, given = shares_of(tp_count, rows)
    alone = tp_count * parts - late
    dp = lax.axis_index("dp")
    z, core = dp // CORES, dp % CORES
    ends = (z == 0) | (z == planes - 1)

    def put(ref, n, owner, unit, sem):
        here = far_unit(dp_count, tp_count, rows, engine_ref, owner, unit)
        return pltpu.make_async_copy(ref.at[pl.ds(n * part_rows, part_rows), :], here, sems.at[sem])

    copies = []
    for ref, owner in ((late_ref, core), (other_ref, 1 - core)):
        for n in range(ref.shape[0] // part_rows):
            copies.append(put(ref, n, owner, n + skip + both + owner * (alone - both), len(copies)))
    missed = ([], [])
    if len(refs) > 2:
        missed = [
            [put(refs[0], n, *u, len(copies) + n) for n, u in enumerate(unshared_of(tp_count, rows, 1 - mine))]
            for mine in range(CORES)
        ]

    for mine in range(CORES):

        @pl.when(ends & (core == mine))
        def _():
            for cp in copies + missed[mine]:
                cp.start()
            for cp in copies + missed[mine]:
                cp.wait()


def store(dp_count, tp_count, rows, skip, engine, *late):
    count = sum(x.shape[0] for x in late) * parts_of(rows) // rows
    return pl.pallas_call(
        functools.partial(store_kernel, dp_count, tp_count, rows, skip),
        in_specs=[pl.BlockSpec(memory_space=pltpu.HBM)] + [pl.BlockSpec(memory_space=pl.ANY)] * len(late),
        out_specs=pl.BlockSpec(memory_space=pltpu.HBM),
        out_shape=jax.ShapeDtypeStruct(engine.shape, engine.dtype),
        input_output_aliases={0: 0},
        scratch_shapes=[pltpu.SemaphoreType.DMA((count,))],
        compiler_params=pltpu.CompilerParams(vmem_limit_bytes=2**20),
        cost_estimate=pl.CostEstimate(flops=1, bytes_accessed=8 * late[0].size, transcendentals=0),
    )(engine, *[pltpu.with_memory_space_constraint(x, pltpu.VMEM) for x in late])


def body(dp_count, tp_count, *arrays):
    rows = arrays[0].shape[0]
    sizes = dp_count, tp_count, rows
    gathered, *late = spread(dp_count, tp_count, *arrays)
    top = dp_count - CORES
    pairs = [(top - CORES + c, top + c) for c in range(CORES)] + [(CORES + c, c) for c in range(CORES)]
    late = [lax.ppermute(x, "dp", pairs) for x in late]
    new_master, new_avg, new_avg_sq, engine = local_step(arrays, gathered)
    for n, (skip, _) in enumerate(late_pieces(tp_count, rows)):
        late[n], gathered, engine = lax.optimization_barrier((late[n], gathered, engine))
        *missed, other = exchange(*sizes, n + 1, late[n], *([gathered] if n == 0 else []))
        engine = store(*sizes, skip, engine, late[n], other, *missed)
    return new_master, new_avg, new_avg_sq, engine


def solution(mesh):
    flat = P(("dp", "tp"), None)
    return jax.shard_map(
        functools.partial(body, mesh.shape["dp"], mesh.shape["tp"]),
        mesh=mesh,
        in_specs=(flat,) * 4,
        out_specs=(flat, flat, flat, P(None, "tp")),
        check_vma=False,
    )
```

```python
import functools

import jax
import jax.numpy as jnp
from jax import lax
from jax.experimental import pallas as pl
from jax.experimental.pallas import tpu as pltpu
from jax.sharding import PartitionSpec as P

QH = 64
KVH = 8
HS = 128
CORES = 2
STEP = 16
AHEAD = 3
TAIL = (1, 1)
UNSHARED = 1
MESH = pl.DeviceIdType.MESH


def step_math(master, grad, exp_avg, exp_avg_sq):
    corr_one = 1.0 - 0.9**10
    corr_two = 1.0 - 0.999**10
    new_avg = 0.9 * exp_avg + 0.1 * grad
    new_avg_sq = 0.999 * exp_avg_sq + 0.001 * grad * grad
    update = new_avg / corr_one / (jnp.sqrt(new_avg_sq / corr_two) + 1e-08)
    new_master = master - 0.001 * (update + 0.1 * master)
    return new_master, new_avg, new_avg_sq


def pieces_of(tp_count, t):
    q, kv = QH // tp_count * HS, KVH // tp_count * HS
    return [(t * q, q, 0), (QH * HS + t * kv, kv, q), ((QH + KVH) * HS + t * kv, kv, q + kv)]


def mix(t, j, count):
    out, bit = 0, 1
    while bit < count:
        out = out + ((t // bit) % 2 + (j // bit) % 2) % 2 * bit
        bit *= 2
    return out


def parts_of(rows):
    return 2 if rows % 64 == 0 else 1


def jobs_of(tp_count, rows):
    part_rows = rows // parts_of(rows)
    jobs, start = [], 0
    first = [min(2 * STEP, part_rows)]
    while sum(first) < part_rows:
        first.append(min(sum(first), part_rows - sum(first)))
    for size in first + [part_rows] * (rows // part_rows - 1):
        jobs.append((0, start, size))
        start += size
    for j in range(1, tp_count):
        for h in range(rows // part_rows):
            jobs.append((j, h * part_rows, part_rows))
    return jobs


def spread_kernel(dp_count, tp_count, parts, *refs):
    count = 5 + len(late_pieces(tp_count, refs[0].shape[0]))
    sources, (out_ref, *late_refs), (held, mine, load_sem) = refs[:4], refs[4:count], refs[count : count + 3]
    own_sem, late_sem, given_sem, flat_send, up_send, down_send, side_send, in_recv, side_recv = refs[count + 3 :]
    planes = dp_count // CORES
    dp, t = lax.axis_index("dp"), lax.axis_index("tp")
    z, core = dp // CORES, dp % CORES
    rows = mine.shape[1]
    part_rows = rows // parts
    has_up, has_down = z < planes - 1, z > 0
    units = tp_count * parts

    up = {"dp": dp + CORES}
    down = {"dp": dp - CORES}
    side = {"dp": z * CORES + 1 - core}

    barrier = pltpu.get_barrier_semaphore()
    for j in reversed(range(1, tp_count)):
        pl.semaphore_signal(barrier, inc=1, device_id={"tp": mix(t, j, tp_count)}, device_id_type=MESH)
    pl.semaphore_signal(barrier, inc=1, device_id=side, device_id_type=MESH)

    @pl.when(has_up)
    def _():
        pl.semaphore_signal(barrier, inc=1, device_id=up, device_id_type=MESH)

    @pl.when(has_down)
    def _():
        pl.semaphore_signal(barrier, inc=1, device_id=down, device_id_type=MESH)

    jobs, ahead = jobs_of(tp_count, rows), AHEAD

    def loads(i):
        j, first, size = jobs[i]
        part = pl.ds(first, size)
        return [
            pltpu.make_async_copy(
                sources[n].at[part, pl.ds(pl.multiple_of(start, HS), width)],
                held.at[j, n, part, pl.ds(into, width)],
                load_sem.at[i % (ahead + 1)],
            )
            for n in range(4)
            for start, width, into in pieces_of(tp_count, mix(t, j, tp_count))
        ]

    def loaded(i):
        j, first, size = jobs[i]
        all_of_it = held.at[j, :, pl.ds(first, size), :]
        pltpu.make_async_copy(all_of_it, all_of_it, load_sem.at[i % (ahead + 1)]).wait()

    def compute(i):
        j, first, size = jobs[i]

        def rows_at(start):
            part = pl.ds(start, STEP)
            new_master = step_math(*[held[j, n, part, :] for n in range(4)])[0]
            mine[j, part, :] = new_master.astype(jnp.bfloat16)

        if size == STEP:
            rows_at(first)
        else:

            @pl.loop(0, size // STEP)
            def _(k):
                rows_at(pl.multiple_of(first + k * STEP, STEP))

    def place(plane, which_core, unit):
        source = mix(t, unit // parts, tp_count)
        block = (plane * CORES + which_core) * tp_count + source
        start = block * rows + unit % parts * part_rows
        return out_ref.at[pl.ds(pl.multiple_of(start, part_rows), part_rows), :]

    def copy(src, dst, send, recv, target):
        return pltpu.make_async_remote_copy(
            src_ref=src, dst_ref=dst, send_sem=send, recv_sem=recv, device_id=target, device_id_type=MESH
        )

    def going_up(src, dst, plane, unit):
        return copy(src, dst, up_send.at[plane], in_recv.at[plane, unit], up)

    def going_down(src, dst, plane, unit):
        return copy(src, dst, down_send.at[plane], in_recv.at[plane, unit], down)

    def going_side(src, dst, plane, unit):
        return copy(src, dst, side_send.at[plane], side_recv.at[plane], side)

    def arrived(plane, unit):
        here = place(plane, core, unit)
        copy(here, here, side_send.at[plane], in_recv.at[plane, unit], side).wait_recv()

    def home(first, size):
        start = ((z * CORES + core) * tp_count + t) * rows + first
        return out_ref.at[pl.ds(pl.multiple_of(start, STEP), size), :]

    def flat_copy(j, h):
        part = pl.ds(h * part_rows, part_rows)
        unit = j * parts + h
        target = {"tp": mix(t, j, tp_count)}
        return copy(mine.at[j, part, :], home(h * part_rows, part_rows), flat_send.at[0], in_recv.at[z, unit], target)

    def keep(h):
        return pltpu.make_async_copy(mine.at[0, pl.ds(h * part_rows, part_rows), :], place(z, core, h), own_sem.at[0])

    def send(i):
        j, first, size = jobs[i]
        h = first // part_rows
        if j > 0:
            flat_copy(j, h).start()
            return
        src, dst = mine.at[0, pl.ds(first, size), :], home(first, size)

        @pl.when(has_up)
        def _():
            going_up(src, dst, z, h).start()

        @pl.when(has_down)
        def _():
            going_down(src, dst, z, h).start()

        going_side(src, dst, z, h).start()
        if (first + size) % part_rows == 0:
            keep(h).start()

    for i in range(ahead):
        for cp in loads(i):
            cp.start()
    for i in range(len(jobs)):
        loaded(i)
        compute(i)
        if i == 1:
            pl.semaphore_wait(barrier, tp_count + has_up.astype(jnp.int32) + has_down.astype(jnp.int32))
        if i > 0:
            send(i - 1)
        if i + ahead < len(jobs):
            for cp in loads(i + ahead):
                cp.start()
    send(len(jobs) - 1)

    @pl.loop(parts, units)
    def _(unit):
        arrived(z, unit)
        here = place(z, core, unit)

        @pl.when(has_up)
        def _():
            going_up(here, here, z, unit).start()

        @pl.when(has_down)
        def _():
            going_down(here, here, z, unit).start()

        going_side(here, here, z, unit).start()

    both, late, given = shares_of(tp_count, rows)
    alone, shared = units - late, both - UNSHARED
    first = jnp.where(core == 0, both, alone)
    low, high = z == 1, z == planes - 2

    def sum_of(count, send_sem, recv_sem):
        here = out_ref.at[pl.ds(0, count * part_rows), :]
        return copy(here, here, send_sem, recv_sem, side)

    def sides_done(plane, count):
        done = sum_of(count, side_send.at[plane], side_recv.at[plane])
        done.wait_send()
        done.wait_recv()

    def set_aside(here, which, n):
        part = pl.ds(pl.multiple_of(n * part_rows, part_rows), part_rows)
        return pltpu.make_async_copy(here, late_refs[which].at[part, :], late_sem.at[which])

    def set_aside_start(here, n):
        for which, (skip, size) in enumerate(late_pieces(tp_count, rows)):

            @pl.when((n >= skip) & (n < skip + size))
            def _():
                set_aside(here, which, n - skip).start()

    def hand_over(plane, n, target):
        here = place(plane, 0, units - given + n)
        return copy(here, here, given_sem.at[0, n], given_sem.at[1, n], target)

    @pl.loop(units, (planes - 1) * units)
    def _(m):
        distance, unit = m // units, m % units
        below, above = z - distance, z + distance
        keeps = (distance == planes - 2) & (unit >= first)
        aside = keeps & (unit < first + late)

        @pl.when(below >= 0)
        def _():
            arrived(below, unit)
            here = place(below, core, unit)

            @pl.when(has_up & jnp.logical_not(keeps))
            def _():
                going_up(here, here, below, unit).start()

            @pl.when(has_up & aside)
            def _():
                set_aside_start(here, unit - first)

            going_side(here, here, below, unit).start()

        @pl.when(above < planes)
        def _():
            arrived(above, unit)
            here = place(above, core, unit)

            @pl.when(has_down & jnp.logical_not(keeps))
            def _():
                going_down(here, here, above, unit).start()

            @pl.when(has_down & aside)
            def _():
                set_aside_start(here, unit - first)

            going_side(here, here, above, unit).start()

    mine_all, flats = mine.at[0], mine.at[pl.ds(1, tp_count - 1)]
    pltpu.make_async_copy(mine_all, mine_all, own_sem.at[0]).wait()
    copy(flats, flats, flat_send.at[0], side_recv.at[z], side).wait_send()

    @pl.when(has_up)
    def _():
        sum_of(units, up_send.at[z], side_recv.at[z]).wait_send()

    @pl.when(has_down)
    def _():
        sum_of(units, down_send.at[z], side_recv.at[z]).wait_send()

    far = [((z == planes - 1), 0), ((z == 0), planes - 1)]

    @pl.loop(0, planes)
    def _(plane):
        @pl.when((plane - z < planes - 1) & (z - plane < planes - 1))
        def _():
            sides_done(plane, units)

    for starts, plane, target in ((high, 0, up), (low, planes - 1, down)):

        @pl.when(starts & (core == 1))
        def _():
            for n in range(given):
                hand_over(plane, n, target).start()

    for ends, plane in far:

        @pl.when(ends)
        def _():
            @pl.loop(0, shared)
            def _(unit):
                arrived(plane, unit)
                here = place(plane, core, unit)
                going_side(here, here, plane, unit).start()

            @pl.loop(shared, both)
            def _(unit):
                arrived(plane, unit)

            sides_done(plane, shared)

            @pl.when(core == 1)
            def _():
                @pl.loop(both, alone)
                def _(unit):
                    arrived(plane, unit)

                for n in range(given):
                    hand_over(plane, n, side).wait_recv()

    for starts, plane, target, sems in ((high, 0, up, up_send), (low, planes - 1, down, down_send)):

        @pl.when(starts)
        def _():
            for which, ref in enumerate(late_refs):
                pltpu.make_async_copy(ref, ref, late_sem.at[which]).wait()

            for owner, count in ((0, both), (1, alone)):

                @pl.when(core == owner)
                def _():
                    sum_of(count, sems.at[plane], side_recv.at[plane]).wait_send()
                    if owner == 1:
                        for n in range(given):
                            hand_over(plane, n, target).wait_send()

    @pl.loop(0, planes)
    def _(plane):
        @pl.when((plane < z) & has_up & jnp.logical_not((plane == 0) & high))
        def _():
            sum_of(units, up_send.at[plane], side_recv.at[plane]).wait_send()

        @pl.when((plane > z) & has_down & jnp.logical_not((plane == planes - 1) & low))
        def _():
            sum_of(units, down_send.at[plane], side_recv.at[plane]).wait_send()


def shares_of(tp_count, rows):
    units = tp_count * parts_of(rows)
    late, given = units // 2 + 1, 1
    return units - late - given, late, given


def late_pieces(tp_count, rows):
    late = shares_of(tp_count, rows)[1]
    sizes = (late - sum(TAIL),) + TAIL
    return [(sum(sizes[:i]), size) for i, size in enumerate(sizes)]


def spread(dp_count, tp_count, *arrays):
    rows, cols = arrays[0].shape
    width = cols // tp_count
    parts = parts_of(rows)
    planes, units = dp_count // CORES, tp_count * parts
    late, pieces = shares_of(tp_count, rows)[1], late_pieces(tp_count, rows)
    return pl.pallas_call(
        functools.partial(spread_kernel, dp_count, tp_count, parts),
        in_specs=[pl.BlockSpec(memory_space=pltpu.HBM)] * 4,
        out_specs=[pl.BlockSpec(memory_space=pl.ANY)] * (1 + len(pieces)),
        out_shape=[
            pltpu.VMEM((dp_count * tp_count * rows, width), jnp.bfloat16),
        ]
        + [pltpu.VMEM((n * rows // parts, width), jnp.bfloat16) for _, n in pieces],
        scratch_shapes=[
            pltpu.VMEM((tp_count, 4, rows, width), jnp.float32),
            pltpu.VMEM((tp_count, rows, width), jnp.bfloat16),
            pltpu.SemaphoreType.DMA((AHEAD + 1,)),
            pltpu.SemaphoreType.DMA((1,)),
            pltpu.SemaphoreType.DMA((len(pieces),)),
            pltpu.SemaphoreType.DMA((2, shares_of(tp_count, rows)[2])),
            pltpu.SemaphoreType.DMA((1,)),
            pltpu.SemaphoreType.DMA((planes,)),
            pltpu.SemaphoreType.DMA((planes,)),
            pltpu.SemaphoreType.DMA((planes,)),
            pltpu.SemaphoreType.DMA((planes, units)),
            pltpu.SemaphoreType.DMA((planes,)),
        ],
        compiler_params=pltpu.CompilerParams(collective_id=0, has_side_effects=True, vmem_limit_bytes=28 * 2**20),
        cost_estimate=pl.CostEstimate(flops=20 * rows * cols, bytes_accessed=16 * rows * cols, transcendentals=rows * cols),
    )(*[pltpu.with_memory_space_constraint(x, pltpu.HBM) for x in arrays])


def step_kernel(m_ref, g_ref, a_ref, s_ref, all_ref, nm_ref, na_ref, ns_ref, engine_ref, sems):
    count = sems.shape[0]
    rows = engine_ref.shape[0] // count

    def whole(n):
        part = pl.ds(n * rows, rows)
        return pltpu.make_async_copy(all_ref.at[part, :], engine_ref.at[part, :], sems.at[n])

    @pl.when(pl.program_id(0) == 0)
    def _():
        for n in range(count):
            whole(n).start()

    new_master, new_avg, new_avg_sq = step_math(m_ref[...], g_ref[...], a_ref[...], s_ref[...])
    nm_ref[...] = new_master
    na_ref[...] = new_avg
    ns_ref[...] = new_avg_sq

    @pl.when(pl.program_id(0) == pl.num_programs(0) - 1)
    def _():
        for n in range(count):
            whole(n).wait()


def local_step(arrays, gathered):
    rows, cols = arrays[0].shape
    tile = 16
    flat = pl.BlockSpec((tile, cols), lambda i: (i, 0))
    f32 = jax.ShapeDtypeStruct((rows, cols), jnp.float32)
    return pl.pallas_call(
        step_kernel,
        grid=(rows // tile,),
        in_specs=[flat] * 4 + [pl.BlockSpec(memory_space=pl.ANY)],
        out_specs=[flat] * 3 + [pl.BlockSpec(memory_space=pltpu.HBM)],
        out_shape=[f32] * 3 + [jax.ShapeDtypeStruct(gathered.shape, gathered.dtype)],
        scratch_shapes=[pltpu.SemaphoreType.DMA((4,))],
        compiler_params=pltpu.CompilerParams(vmem_limit_bytes=24 * 2**20),
        cost_estimate=pl.CostEstimate(
            flops=20 * rows * cols,
            bytes_accessed=28 * rows * cols + 2 * gathered.size,
            transcendentals=rows * cols,
        ),
    )(*[pltpu.with_memory_space_constraint(x, pltpu.HBM) for x in arrays], pltpu.with_memory_space_constraint(gathered, pltpu.VMEM))


def far_unit(dp_count, tp_count, rows, ref, owner, unit):
    planes, parts = dp_count // CORES, parts_of(rows)
    part_rows = rows // parts
    z, t = lax.axis_index("dp") // CORES, lax.axis_index("tp")
    block = ((planes - 1 - z) * CORES + owner) * tp_count + mix(t, unit // parts, tp_count)
    start = block * rows + unit % parts * part_rows
    return ref.at[pl.ds(pl.multiple_of(start, part_rows), part_rows), :]


def unshared_of(tp_count, rows, core):
    both, late, given = shares_of(tp_count, rows)
    units = tp_count * parts_of(rows)
    if core == 0:
        return [(0, unit) for unit in range(both - UNSHARED, both)]
    return [(1, unit) for unit in range(both - UNSHARED, units - late)] + [(0, unit) for unit in range(units - given, units)]


def greet(side):
    barrier = pltpu.get_barrier_semaphore()
    pl.semaphore_signal(barrier, inc=1, device_id=side, device_id_type=MESH)
    pl.semaphore_wait(barrier, 1)


def exchange_kernel(dp_count, tp_count, rows, *refs):
    planes, part_rows = dp_count // CORES, rows // parts_of(rows)
    dp = lax.axis_index("dp")
    z, core = dp // CORES, dp % CORES
    side = {"dp": z * CORES + 1 - core}
    greet(side)
    late_ref, other_ref, send_sems, recv_sems = refs[0], refs[-3], refs[-2], refs[-1]

    def copy(src, dst, n):
        return pltpu.make_async_remote_copy(
            src_ref=src,
            dst_ref=dst,
            send_sem=send_sems.at[n],
            recv_sem=recv_sems.at[n],
            device_id=side,
            device_id_type=MESH,
        )

    both_ways = copy(late_ref, other_ref, 0)
    missed = ([], [])
    if len(refs) > 4:
        all_ref, missed_ref = refs[1:3]
        for owner_core, copies in enumerate(missed):
            for n, (owner, unit) in enumerate(unshared_of(tp_count, rows, owner_core)):
                src = far_unit(dp_count, tp_count, rows, all_ref, owner, unit)
                copies.append(copy(src, missed_ref.at[pl.ds(n * part_rows, part_rows), :], n + 1))

    @pl.when((z == 0) | (z == planes - 1))
    def _():
        for mine in range(CORES):

            @pl.when(core == mine)
            def _():
                for cp in missed[mine]:
                    cp.start()
                both_ways.start()
                for cp in missed[mine]:
                    cp.wait_send()
                for cp in missed[1 - mine]:
                    cp.wait_recv()

        both_ways.wait()


def exchange(dp_count, tp_count, rows, number, arrived, *gathered):
    shapes = [arrived.shape]
    if gathered:
        shapes.insert(0, (len(unshared_of(tp_count, rows, 1)) * rows // parts_of(rows), arrived.shape[1]))
    copies = 1 + len(unshared_of(tp_count, rows, 1)) * len(gathered)
    return pl.pallas_call(
        functools.partial(exchange_kernel, dp_count, tp_count, rows),
        in_specs=[pl.BlockSpec(memory_space=pl.ANY)] * (1 + len(gathered)),
        out_specs=[pl.BlockSpec(memory_space=pl.ANY)] * len(shapes),
        out_shape=[pltpu.VMEM(shape, arrived.dtype) for shape in shapes],
        scratch_shapes=[pltpu.SemaphoreType.DMA((copies,))] * 2,
        compiler_params=pltpu.CompilerParams(collective_id=number, has_side_effects=True, vmem_limit_bytes=2**20),
        cost_estimate=pl.CostEstimate(flops=1, bytes_accessed=4 * arrived.size, transcendentals=0),
    )(*[pltpu.with_memory_space_constraint(x, pltpu.VMEM) for x in (arrived, *gathered)])


def store_kernel(dp_count, tp_count, rows, skip, _, late_ref, other_ref, *refs):
    engine_ref, sems = refs[-2:]
    planes, parts = dp_count // CORES, parts_of(rows)
    part_rows = rows // parts
    both, late, given = shares_of(tp_count, rows)
    alone = tp_count * parts - late
    dp = lax.axis_index("dp")
    z, core = dp // CORES, dp % CORES
    ends = (z == 0) | (z == planes - 1)

    def put(ref, n, owner, unit, sem):
        here = far_unit(dp_count, tp_count, rows, engine_ref, owner, unit)
        return pltpu.make_async_copy(ref.at[pl.ds(n * part_rows, part_rows), :], here, sems.at[sem])

    copies = []
    for ref, owner in ((late_ref, core), (other_ref, 1 - core)):
        for n in range(ref.shape[0] // part_rows):
            copies.append(put(ref, n, owner, n + skip + both + owner * (alone - both), len(copies)))
    missed = ([], [])
    if len(refs) > 2:
        missed = [
            [put(refs[0], n, *u, len(copies) + n) for n, u in enumerate(unshared_of(tp_count, rows, 1 - mine))]
            for mine in range(CORES)
        ]

    for mine in range(CORES):

        @pl.when(ends & (core == mine))
        def _():
            for cp in copies + missed[mine]:
                cp.start()
            for cp in copies + missed[mine]:
                cp.wait()


def store(dp_count, tp_count, rows, skip, engine, *late):
    count = sum(x.shape[0] for x in late) * parts_of(rows) // rows
    return pl.pallas_call(
        functools.partial(store_kernel, dp_count, tp_count, rows, skip),
        in_specs=[pl.BlockSpec(memory_space=pltpu.HBM)] + [pl.BlockSpec(memory_space=pl.ANY)] * len(late),
        out_specs=pl.BlockSpec(memory_space=pltpu.HBM),
        out_shape=jax.ShapeDtypeStruct(engine.shape, engine.dtype),
        input_output_aliases={0: 0},
        scratch_shapes=[pltpu.SemaphoreType.DMA((count,))],
        compiler_params=pltpu.CompilerParams(vmem_limit_bytes=2**20),
        cost_estimate=pl.CostEstimate(flops=1, bytes_accessed=8 * late[0].size, transcendentals=0),
    )(engine, *[pltpu.with_memory_space_constraint(x, pltpu.VMEM) for x in late])


def body(dp_count, tp_count, *arrays):
    rows = arrays[0].shape[0]
    sizes = dp_count, tp_count, rows
    gathered, *late = spread(dp_count, tp_count, *arrays)
    top = dp_count - CORES
    pairs = [(top - CORES + c, top + c) for c in range(CORES)] + [(CORES + c, c) for c in range(CORES)]
    late = [lax.ppermute(x, "dp", pairs) for x in late]
    new_master, new_avg, new_avg_sq, engine = local_step(arrays, gathered)
    for n, (skip, _) in enumerate(late_pieces(tp_count, rows)):
        late[n], gathered, engine = lax.optimization_barrier((late[n], gathered, engine))
        *missed, other = exchange(*sizes, n + 1, late[n], *([gathered] if n == 0 else []))
        engine = store(*sizes, skip, engine, late[n], other, *missed)
    return new_master, new_avg, new_avg_sq, engine


def solution(mesh):
    flat = P(("dp", "tp"), None)
    return jax.shard_map(
        functools.partial(body, mesh.shape["dp"], mesh.shape["tp"]),
        mesh=mesh,
        in_specs=(flat,) * 4,
        out_specs=(flat, flat, flat, P(None, "tp")),
        check_vma=False,
    )
```

```python
import functools

import jax
import jax.numpy as jnp
from jax import lax
from jax.experimental import pallas as pl
from jax.experimental.pallas import tpu as pltpu
from jax.sharding import PartitionSpec as P

QH = 64
KVH = 8
HS = 128
CORES = 2
STEP = 16
AHEAD = 3
TAIL = (2, 1)
MESH = pl.DeviceIdType.MESH


def step_math(master, grad, exp_avg, exp_avg_sq):
    corr_one = 1.0 - 0.9**10
    corr_two = 1.0 - 0.999**10
    new_avg = 0.9 * exp_avg + 0.1 * grad
    new_avg_sq = 0.999 * exp_avg_sq + 0.001 * grad * grad
    update = new_avg / corr_one / (jnp.sqrt(new_avg_sq / corr_two) + 1e-08)
    new_master = master - 0.001 * (update + 0.1 * master)
    return new_master, new_avg, new_avg_sq


def pieces_of(tp_count, t):
    q, kv = QH // tp_count * HS, KVH // tp_count * HS
    return [(t * q, q, 0), (QH * HS + t * kv, kv, q), ((QH + KVH) * HS + t * kv, kv, q + kv)]


def mix(t, j, count):
    out, bit = 0, 1
    while bit < count:
        out = out + ((t // bit) % 2 + (j // bit) % 2) % 2 * bit
        bit *= 2
    return out


def parts_of(rows):
    return 2 if rows % 64 == 0 else 1


def jobs_of(tp_count, rows):
    part_rows = rows // parts_of(rows)
    jobs, start = [], 0
    first = [STEP, STEP]
    while sum(first) < part_rows:
        first.append(min(sum(first), part_rows - sum(first)))
    for size in first + [part_rows] * (rows // part_rows - 1):
        jobs.append((0, start, size))
        start += size
    for j in range(1, tp_count):
        for h in range(rows // part_rows):
            jobs.append((j, h * part_rows, part_rows))
    return jobs


def spread_kernel(dp_count, tp_count, parts, *refs):
    count = 5 + len(late_pieces(tp_count, refs[0].shape[0]))
    sources, (out_ref, *late_refs), (held, mine, load_sem) = refs[:4], refs[4:count], refs[count : count + 3]
    own_sem, late_sem, given_sem, flat_send, up_send, down_send, side_send, in_recv, side_recv = refs[count + 3 :]
    planes = dp_count // CORES
    dp, t = lax.axis_index("dp"), lax.axis_index("tp")
    z, core = dp // CORES, dp % CORES
    rows = mine.shape[1]
    part_rows = rows // parts
    has_up, has_down = z < planes - 1, z > 0
    units = tp_count * parts

    up = {"dp": dp + CORES}
    down = {"dp": dp - CORES}
    side = {"dp": z * CORES + 1 - core}

    barrier = pltpu.get_barrier_semaphore()
    for j in reversed(range(1, tp_count)):
        pl.semaphore_signal(barrier, inc=1, device_id={"tp": mix(t, j, tp_count)}, device_id_type=MESH)
    pl.semaphore_signal(barrier, inc=1, device_id=side, device_id_type=MESH)

    @pl.when(has_up)
    def _():
        pl.semaphore_signal(barrier, inc=1, device_id=up, device_id_type=MESH)

    @pl.when(has_down)
    def _():
        pl.semaphore_signal(barrier, inc=1, device_id=down, device_id_type=MESH)

    jobs, ahead = jobs_of(tp_count, rows), AHEAD

    def loads(i):
        j, first, size = jobs[i]
        part = pl.ds(first, size)
        return [
            pltpu.make_async_copy(
                sources[n].at[part, pl.ds(pl.multiple_of(start, HS), width)],
                held.at[j, n, part, pl.ds(into, width)],
                load_sem.at[i % (ahead + 1)],
            )
            for n in range(4)
            for start, width, into in pieces_of(tp_count, mix(t, j, tp_count))
        ]

    def loaded(i):
        j, first, size = jobs[i]
        all_of_it = held.at[j, :, pl.ds(first, size), :]
        pltpu.make_async_copy(all_of_it, all_of_it, load_sem.at[i % (ahead + 1)]).wait()

    def compute(i):
        j, first, size = jobs[i]

        def rows_at(start):
            part = pl.ds(start, STEP)
            new_master = step_math(*[held[j, n, part, :] for n in range(4)])[0]
            mine[j, part, :] = new_master.astype(jnp.bfloat16)

        if size == STEP:
            rows_at(first)
        else:

            @pl.loop(0, size // STEP)
            def _(k):
                rows_at(pl.multiple_of(first + k * STEP, STEP))

    def place(plane, which_core, unit):
        source = mix(t, unit // parts, tp_count)
        block = (plane * CORES + which_core) * tp_count + source
        start = block * rows + unit % parts * part_rows
        return out_ref.at[pl.ds(pl.multiple_of(start, part_rows), part_rows), :]

    def copy(src, dst, send, recv, target):
        return pltpu.make_async_remote_copy(
            src_ref=src, dst_ref=dst, send_sem=send, recv_sem=recv, device_id=target, device_id_type=MESH
        )

    def going_up(src, dst, plane, unit):
        return copy(src, dst, up_send.at[plane], in_recv.at[plane, unit], up)

    def going_down(src, dst, plane, unit):
        return copy(src, dst, down_send.at[plane], in_recv.at[plane, unit], down)

    def going_side(src, dst, plane, unit):
        return copy(src, dst, side_send.at[plane], side_recv.at[plane], side)

    def arrived(plane, unit):
        here = place(plane, core, unit)
        copy(here, here, side_send.at[plane], in_recv.at[plane, unit], side).wait_recv()

    def home(first, size):
        start = ((z * CORES + core) * tp_count + t) * rows + first
        return out_ref.at[pl.ds(pl.multiple_of(start, STEP), size), :]

    def flat_copy(j, h):
        part = pl.ds(h * part_rows, part_rows)
        unit = j * parts + h
        target = {"tp": mix(t, j, tp_count)}
        return copy(mine.at[j, part, :], home(h * part_rows, part_rows), flat_send.at[0], in_recv.at[z, unit], target)

    def keep(h):
        return pltpu.make_async_copy(mine.at[0, pl.ds(h * part_rows, part_rows), :], place(z, core, h), own_sem.at[0])

    def send(i):
        j, first, size = jobs[i]
        h = first // part_rows
        if j > 0:
            flat_copy(j, h).start()
            return
        src, dst = mine.at[0, pl.ds(first, size), :], home(first, size)

        @pl.when(has_up)
        def _():
            going_up(src, dst, z, h).start()

        @pl.when(has_down)
        def _():
            going_down(src, dst, z, h).start()

        going_side(src, dst, z, h).start()
        if (first + size) % part_rows == 0:
            keep(h).start()

    for i in range(ahead):
        for cp in loads(i):
            cp.start()
    for i in range(len(jobs)):
        loaded(i)
        compute(i)
        if i == 1:
            pl.semaphore_wait(barrier, tp_count + has_up.astype(jnp.int32) + has_down.astype(jnp.int32))
        if i > 0:
            send(i - 1)
        if i + ahead < len(jobs):
            for cp in loads(i + ahead):
                cp.start()
    send(len(jobs) - 1)

    @pl.loop(parts, units)
    def _(unit):
        arrived(z, unit)
        here = place(z, core, unit)

        @pl.when(has_up)
        def _():
            going_up(here, here, z, unit).start()

        @pl.when(has_down)
        def _():
            going_down(here, here, z, unit).start()

        going_side(here, here, z, unit).start()

    both, late, given = shares_of(tp_count, rows)
    alone = units - late
    first = jnp.where(core == 0, both, alone)
    low, high = z == 1, z == planes - 2

    def sum_of(count, send_sem, recv_sem):
        here = out_ref.at[pl.ds(0, count * part_rows), :]
        return copy(here, here, send_sem, recv_sem, side)

    def sides_done(plane, count):
        done = sum_of(count, side_send.at[plane], side_recv.at[plane])
        done.wait_send()
        done.wait_recv()

    def set_aside(here, which, n):
        part = pl.ds(pl.multiple_of(n * part_rows, part_rows), part_rows)
        return pltpu.make_async_copy(here, late_refs[which].at[part, :], late_sem.at[which])

    def set_aside_start(here, n):
        for which, (skip, size) in enumerate(late_pieces(tp_count, rows)):

            @pl.when((n >= skip) & (n < skip + size))
            def _():
                set_aside(here, which, n - skip).start()

    def hand_over(plane, n, target):
        here = place(plane, 0, units - given + n)
        return copy(here, here, given_sem.at[0, n], given_sem.at[1, n], target)

    @pl.loop(units, (planes - 1) * units)
    def _(m):
        distance, unit = m // units, m % units
        below, above = z - distance, z + distance
        keeps = (distance == planes - 2) & (unit >= first)
        aside = keeps & (unit < first + late)

        @pl.when(below >= 0)
        def _():
            arrived(below, unit)
            here = place(below, core, unit)

            @pl.when(has_up & jnp.logical_not(keeps))
            def _():
                going_up(here, here, below, unit).start()

            @pl.when(has_up & aside)
            def _():
                set_aside_start(here, unit - first)

            going_side(here, here, below, unit).start()

        @pl.when(above < planes)
        def _():
            arrived(above, unit)
            here = place(above, core, unit)

            @pl.when(has_down & jnp.logical_not(keeps))
            def _():
                going_down(here, here, above, unit).start()

            @pl.when(has_down & aside)
            def _():
                set_aside_start(here, unit - first)

            going_side(here, here, above, unit).start()

    mine_all, flats = mine.at[0], mine.at[pl.ds(1, tp_count - 1)]
    pltpu.make_async_copy(mine_all, mine_all, own_sem.at[0]).wait()
    copy(flats, flats, flat_send.at[0], side_recv.at[z], side).wait_send()

    @pl.when(has_up)
    def _():
        sum_of(units, up_send.at[z], side_recv.at[z]).wait_send()

    @pl.when(has_down)
    def _():
        sum_of(units, down_send.at[z], side_recv.at[z]).wait_send()

    far = [((z == planes - 1), 0), ((z == 0), planes - 1)]

    @pl.loop(0, planes)
    def _(plane):
        @pl.when((plane - z < planes - 1) & (z - plane < planes - 1))
        def _():
            sides_done(plane, units)

    for starts, plane, target in ((high, 0, up), (low, planes - 1, down)):

        @pl.when(starts & (core == 1))
        def _():
            for n in range(given):
                hand_over(plane, n, target).start()

    for ends, plane in far:

        @pl.when(ends)
        def _():
            @pl.loop(0, both)
            def _(unit):
                arrived(plane, unit)

            @pl.when(core == 1)
            def _():
                @pl.loop(both, alone)
                def _(unit):
                    arrived(plane, unit)

                for n in range(given):
                    hand_over(plane, n, side).wait_recv()

    for starts, plane, target, sems in ((high, 0, up, up_send), (low, planes - 1, down, down_send)):

        @pl.when(starts)
        def _():
            for which, ref in enumerate(late_refs):
                pltpu.make_async_copy(ref, ref, late_sem.at[which]).wait()

            for owner, count in ((0, both), (1, alone)):

                @pl.when(core == owner)
                def _():
                    sum_of(count, sems.at[plane], side_recv.at[plane]).wait_send()
                    if owner == 1:
                        for n in range(given):
                            hand_over(plane, n, target).wait_send()

    @pl.loop(0, planes)
    def _(plane):
        @pl.when((plane < z) & has_up & jnp.logical_not((plane == 0) & high))
        def _():
            sum_of(units, up_send.at[plane], side_recv.at[plane]).wait_send()

        @pl.when((plane > z) & has_down & jnp.logical_not((plane == planes - 1) & low))
        def _():
            sum_of(units, down_send.at[plane], side_recv.at[plane]).wait_send()


def shares_of(tp_count, rows):
    units = tp_count * parts_of(rows)
    late, given = units // 2 + 2, 1
    return units - late - given, late, given


def late_pieces(tp_count, rows):
    late = shares_of(tp_count, rows)[1]
    sizes = (late - sum(TAIL),) + TAIL
    return [(sum(sizes[:i]), size) for i, size in enumerate(sizes)]


def spread(dp_count, tp_count, *arrays):
    rows, cols = arrays[0].shape
    width = cols // tp_count
    parts = parts_of(rows)
    planes, units = dp_count // CORES, tp_count * parts
    late, pieces = shares_of(tp_count, rows)[1], late_pieces(tp_count, rows)
    return pl.pallas_call(
        functools.partial(spread_kernel, dp_count, tp_count, parts),
        in_specs=[pl.BlockSpec(memory_space=pltpu.HBM)] * 4,
        out_specs=[pl.BlockSpec(memory_space=pl.ANY)] * (1 + len(pieces)),
        out_shape=[
            pltpu.VMEM((dp_count * tp_count * rows, width), jnp.bfloat16),
        ]
        + [pltpu.VMEM((n * rows // parts, width), jnp.bfloat16) for _, n in pieces],
        scratch_shapes=[
            pltpu.VMEM((tp_count, 4, rows, width), jnp.float32),
            pltpu.VMEM((tp_count, rows, width), jnp.bfloat16),
            pltpu.SemaphoreType.DMA((AHEAD + 1,)),
            pltpu.SemaphoreType.DMA((1,)),
            pltpu.SemaphoreType.DMA((len(pieces),)),
            pltpu.SemaphoreType.DMA((2, shares_of(tp_count, rows)[2])),
            pltpu.SemaphoreType.DMA((1,)),
            pltpu.SemaphoreType.DMA((planes,)),
            pltpu.SemaphoreType.DMA((planes,)),
            pltpu.SemaphoreType.DMA((planes,)),
            pltpu.SemaphoreType.DMA((planes, units)),
            pltpu.SemaphoreType.DMA((planes,)),
        ],
        compiler_params=pltpu.CompilerParams(collective_id=0, has_side_effects=True, vmem_limit_bytes=28 * 2**20),
        cost_estimate=pl.CostEstimate(flops=20 * rows * cols, bytes_accessed=16 * rows * cols, transcendentals=rows * cols),
    )(*[pltpu.with_memory_space_constraint(x, pltpu.HBM) for x in arrays])


def step_kernel(m_ref, g_ref, a_ref, s_ref, all_ref, nm_ref, na_ref, ns_ref, engine_ref, sems):
    count = sems.shape[0]
    rows = engine_ref.shape[0] // count

    def whole(n):
        part = pl.ds(n * rows, rows)
        return pltpu.make_async_copy(all_ref.at[part, :], engine_ref.at[part, :], sems.at[n])

    @pl.when(pl.program_id(0) == 0)
    def _():
        for n in range(count):
            whole(n).start()

    new_master, new_avg, new_avg_sq = step_math(m_ref[...], g_ref[...], a_ref[...], s_ref[...])
    nm_ref[...] = new_master
    na_ref[...] = new_avg
    ns_ref[...] = new_avg_sq

    @pl.when(pl.program_id(0) == pl.num_programs(0) - 1)
    def _():
        for n in range(count):
            whole(n).wait()


def local_step(arrays, gathered):
    rows, cols = arrays[0].shape
    tile = 16
    flat = pl.BlockSpec((tile, cols), lambda i: (i, 0))
    f32 = jax.ShapeDtypeStruct((rows, cols), jnp.float32)
    return pl.pallas_call(
        step_kernel,
        grid=(rows // tile,),
        in_specs=[flat] * 4 + [pl.BlockSpec(memory_space=pl.ANY)],
        out_specs=[flat] * 3 + [pl.BlockSpec(memory_space=pltpu.HBM)],
        out_shape=[f32] * 3 + [jax.ShapeDtypeStruct(gathered.shape, gathered.dtype)],
        scratch_shapes=[pltpu.SemaphoreType.DMA((4,))],
        compiler_params=pltpu.CompilerParams(vmem_limit_bytes=24 * 2**20),
        cost_estimate=pl.CostEstimate(
            flops=20 * rows * cols,
            bytes_accessed=28 * rows * cols + 2 * gathered.size,
            transcendentals=rows * cols,
        ),
    )(*[pltpu.with_memory_space_constraint(x, pltpu.HBM) for x in arrays], pltpu.with_memory_space_constraint(gathered, pltpu.VMEM))


def far_unit(dp_count, tp_count, rows, ref, owner, unit):
    planes, parts = dp_count // CORES, parts_of(rows)
    part_rows = rows // parts
    z, t = lax.axis_index("dp") // CORES, lax.axis_index("tp")
    block = ((planes - 1 - z) * CORES + owner) * tp_count + mix(t, unit // parts, tp_count)
    start = block * rows + unit % parts * part_rows
    return ref.at[pl.ds(pl.multiple_of(start, part_rows), part_rows), :]


def unshared_of(tp_count, rows, core):
    both, late, given = shares_of(tp_count, rows)
    units = tp_count * parts_of(rows)
    if core == 0:
        return [(0, unit) for unit in range(both)]
    return [(1, unit) for unit in range(units - late)] + [(0, unit) for unit in range(units - given, units)]


def greet(side):
    barrier = pltpu.get_barrier_semaphore()
    pl.semaphore_signal(barrier, inc=1, device_id=side, device_id_type=MESH)
    pl.semaphore_wait(barrier, 1)


def exchange_kernel(dp_count, tp_count, rows, *refs):
    planes, part_rows = dp_count // CORES, rows // parts_of(rows)
    dp = lax.axis_index("dp")
    z, core = dp // CORES, dp % CORES
    side = {"dp": z * CORES + 1 - core}
    greet(side)
    late_ref, other_ref, send_sems, recv_sems = refs[0], refs[-3], refs[-2], refs[-1]

    def copy(src, dst, n):
        return pltpu.make_async_remote_copy(
            src_ref=src,
            dst_ref=dst,
            send_sem=send_sems.at[n],
            recv_sem=recv_sems.at[n],
            device_id=side,
            device_id_type=MESH,
        )

    both_ways = copy(late_ref, other_ref, 0)
    missed = ([], [])
    if len(refs) > 4:
        all_ref, missed_ref = refs[1:3]
        for owner_core, copies in enumerate(missed):
            for n, (owner, unit) in enumerate(unshared_of(tp_count, rows, owner_core)):
                src = far_unit(dp_count, tp_count, rows, all_ref, owner, unit)
                copies.append(copy(src, missed_ref.at[pl.ds(n * part_rows, part_rows), :], n + 1))

    @pl.when((z == 0) | (z == planes - 1))
    def _():
        for mine in range(CORES):

            @pl.when(core == mine)
            def _():
                for cp in missed[mine]:
                    cp.start()
                both_ways.start()
                for cp in missed[mine]:
                    cp.wait_send()
                for cp in missed[1 - mine]:
                    cp.wait_recv()

        both_ways.wait()


def exchange(dp_count, tp_count, rows, number, arrived, *gathered):
    shapes = [arrived.shape]
    if gathered:
        shapes.insert(0, (len(unshared_of(tp_count, rows, 1)) * rows // parts_of(rows), arrived.shape[1]))
    copies = 1 + len(unshared_of(tp_count, rows, 1)) * len(gathered)
    return pl.pallas_call(
        functools.partial(exchange_kernel, dp_count, tp_count, rows),
        in_specs=[pl.BlockSpec(memory_space=pl.ANY)] * (1 + len(gathered)),
        out_specs=[pl.BlockSpec(memory_space=pl.ANY)] * len(shapes),
        out_shape=[pltpu.VMEM(shape, arrived.dtype) for shape in shapes],
        scratch_shapes=[pltpu.SemaphoreType.DMA((copies,))] * 2,
        compiler_params=pltpu.CompilerParams(collective_id=number, has_side_effects=True, vmem_limit_bytes=2**20),
        cost_estimate=pl.CostEstimate(flops=1, bytes_accessed=4 * arrived.size, transcendentals=0),
    )(*[pltpu.with_memory_space_constraint(x, pltpu.VMEM) for x in (arrived, *gathered)])


def store_kernel(dp_count, tp_count, rows, skip, _, late_ref, other_ref, *refs):
    engine_ref, sems = refs[-2:]
    planes, parts = dp_count // CORES, parts_of(rows)
    part_rows = rows // parts
    both, late, given = shares_of(tp_count, rows)
    alone = tp_count * parts - late
    dp = lax.axis_index("dp")
    z, core = dp // CORES, dp % CORES
    ends = (z == 0) | (z == planes - 1)

    def put(ref, n, owner, unit, sem):
        here = far_unit(dp_count, tp_count, rows, engine_ref, owner, unit)
        return pltpu.make_async_copy(ref.at[pl.ds(n * part_rows, part_rows), :], here, sems.at[sem])

    copies = []
    for ref, owner in ((late_ref, core), (other_ref, 1 - core)):
        for n in range(ref.shape[0] // part_rows):
            copies.append(put(ref, n, owner, n + skip + both + owner * (alone - both), len(copies)))
    missed = ([], [])
    if len(refs) > 2:
        missed = [
            [put(refs[0], n, *u, len(copies) + n) for n, u in enumerate(unshared_of(tp_count, rows, 1 - mine))]
            for mine in range(CORES)
        ]

    for mine in range(CORES):

        @pl.when(ends & (core == mine))
        def _():
            for cp in copies + missed[mine]:
                cp.start()
            for cp in copies + missed[mine]:
                cp.wait()


def store(dp_count, tp_count, rows, skip, engine, *late):
    count = sum(x.shape[0] for x in late) * parts_of(rows) // rows
    return pl.pallas_call(
        functools.partial(store_kernel, dp_count, tp_count, rows, skip),
        in_specs=[pl.BlockSpec(memory_space=pltpu.HBM)] + [pl.BlockSpec(memory_space=pl.ANY)] * len(late),
        out_specs=pl.BlockSpec(memory_space=pltpu.HBM),
        out_shape=jax.ShapeDtypeStruct(engine.shape, engine.dtype),
        input_output_aliases={0: 0},
        scratch_shapes=[pltpu.SemaphoreType.DMA((count,))],
        compiler_params=pltpu.CompilerParams(vmem_limit_bytes=2**20),
        cost_estimate=pl.CostEstimate(flops=1, bytes_accessed=8 * late[0].size, transcendentals=0),
    )(engine, *[pltpu.with_memory_space_constraint(x, pltpu.VMEM) for x in late])


def body(dp_count, tp_count, *arrays):
    rows = arrays[0].shape[0]
    sizes = dp_count, tp_count, rows
    gathered, *late = spread(dp_count, tp_count, *arrays)
    top = dp_count - CORES
    pairs = [(top - CORES + c, top + c) for c in range(CORES)] + [(CORES + c, c) for c in range(CORES)]
    late = [lax.ppermute(x, "dp", pairs) for x in late]
    new_master, new_avg, new_avg_sq, engine = local_step(arrays, gathered)
    for n, (skip, _) in enumerate(late_pieces(tp_count, rows)):
        late[n], gathered, engine = lax.optimization_barrier((late[n], gathered, engine))
        *missed, other = exchange(*sizes, n + 1, late[n], *([gathered] if n == 0 else []))
        engine = store(*sizes, skip, engine, late[n], other, *missed)
    return new_master, new_avg, new_avg_sq, engine


def solution(mesh):
    flat = P(("dp", "tp"), None)
    return jax.shard_map(
        functools.partial(body, mesh.shape["dp"], mesh.shape["tp"]),
        mesh=mesh,
        in_specs=(flat,) * 4,
        out_specs=(flat, flat, flat, P(None, "tp")),
        check_vma=False,
    )
```
